32 devices in a mesh: rows: 8 (over z, x), width: 4 (over y, core).
Axes of the slice: x: 2, y: 2, z: 4, core: 2. Of those that a mesh axis runs over, the one named last changes fastest.
Arguments:
- w_gate: float32 [3072, 8192], P('rows', 'width'), may hold values from -0.15625 to 0.15625
- avg_gate: float32 [3072, 8192], P('rows', 'width'), may hold values from -0.109375 to 0.109375
- w_up: float32 [3072, 8192], P('rows', 'width'), may hold values from -0.15625 to 0.15625
- avg_up: float32 [3072, 8192], P('rows', 'width'), may hold values from -0.109375 to 0.109375
- norm_gain: float32 [3072], P('rows'), may hold values from 0.25 to 1.75
Outputs:
- serve_gate: bfloat16 [3072, 8192], P(None, 'width')
- serve_up: bfloat16 [3072, 8192], P(None, 'width')
- factor_gate: float32 [8192], P('width')
- factor_up: float32 [8192], P('width')
The draws below stay inside these ranges and needn't reach their ends.
All inputs are finite; a program needn't handle non-finite values. Where the reference program divides by a largest or mean magnitude, that divisor is 1e-20 or more.
Results may differ from the reference program's by a relative error of at most 0.001.
Values may be sent and summed in bfloat16 or wider, within the bound.
No kernel may reach another device: no remote copies, remote signals or barrier semaphores. Data moves between devices by JAX's collectives and lax.ppermute only.
A program may use at most 128 MiB of HBM per device.

```python
import jax
import jax.numpy as jnp

D_MODEL = 3072
D_INNER = 8192


def with_spikes(drawn, rng, source, target, parts, factor):
    owner, partner = [(jnp.arange(drawn.shape[axis_at]) // (drawn.shape[axis_at] // parts)).reshape([-1 if axis == axis_at else 1 for axis in range(drawn.ndim)]) for axis_at in (source, target)]
    chosen = jax.random.permutation(rng, parts)[partner]
    strong = (owner == chosen) | (owner == (partner + parts // 2) % parts)
    return jnp.where(strong, factor * drawn, drawn)


def block_scale(stream_key, extent, shards, low, top_value):
    factor_of, own = 1.0, jax.random.fold_in(stream_key, 6)
    for axis_at, shards_of in shards:
        draws = jnp.exp(jax.random.uniform(jax.random.fold_in(own, axis_at), (shards_of,), jnp.float32, low / len(shards), top_value / len(shards)))
        factor_of = factor_of * jnp.repeat(draws, extent[axis_at] // shards_of).reshape([-1 if axis == axis_at else 1 for axis in range(len(extent))])
    return factor_of


def bell_draw(rng, shape, width, limit, split=(), kind=jnp.bfloat16):
    result = jax.random.normal(rng, shape, jnp.float32) * width
    if len(split) > 0:
        result = block_scale(rng, shape, split, -0.22, 0.18) * result
    return jnp.clip(result, min=-limit, max=limit).astype(kind)


def bell_draw_with(stream_key, extent, spread, reach, pieces, heavy, held_as=jnp.bfloat16):
    values = spread * jax.random.normal(stream_key, extent, jnp.float32)
    if pieces:
        values = values * block_scale(stream_key, extent, pieces, -0.22, 0.18)
    return jnp.clip(with_spikes(values, jax.random.fold_in(stream_key, 3), *heavy), -reach, reach).astype(held_as)


def setup_inputs(seed: int = 0) -> dict:
    keys = jax.random.split(jax.random.key(seed), 6)
    return {
        "w_gate": bell_draw_with(keys[0], (D_MODEL, D_INNER), D_MODEL ** -0.5, 0.15625, ((0, 8), (1, 4)), (0, 1, 8, 2.0), jnp.float32),
        "avg_gate": bell_draw(keys[1], (D_MODEL, D_INNER), D_MODEL ** -0.5, 0.109375, ((0, 8), (1, 4)), jnp.float32),
        "w_up": bell_draw_with(keys[2], (D_MODEL, D_INNER), D_MODEL ** -0.5, 0.15625, ((0, 8), (1, 4)), (0, 1, 8, 2.0), jnp.float32),
        "avg_up": bell_draw(keys[3], (D_MODEL, D_INNER), D_MODEL ** -0.5, 0.109375, ((0, 8), (1, 4)), jnp.float32),
        "norm_gain": jnp.clip(1.0 + 0.15 * jax.random.normal(keys[4], (D_MODEL,), jnp.float32), 0.25, 1.75),
    }


keep_rate = 0.7


def reference(w_gate, avg_gate, w_up, avg_up, norm_gain):
    fresh_gate = keep_rate * avg_gate + (1.0 - keep_rate) * w_gate
    fresh_up = keep_rate * avg_up + (1.0 - keep_rate) * w_up
    fresh_gained_gate = fresh_gate * norm_gain[:, None]
    fresh_gained_up = fresh_up * norm_gain[:, None]
    factor_gate = jnp.max(jnp.abs(fresh_gained_gate), axis=0)
    serve_gate = (fresh_gained_gate / factor_gate).astype(jnp.bfloat16)
    factor_up = jnp.max(jnp.abs(fresh_gained_up), axis=0)
    serve_up = (fresh_gained_up / factor_up).astype(jnp.bfloat16)
    return serve_gate, serve_up, factor_gate, factor_up
```

```python
import functools

import jax
import jax.numpy as jnp
from jax import lax
from jax.experimental import pallas as pl
from jax.experimental.pallas import tpu as pltpu
from jax.sharding import PartitionSpec as P


keep_rate = 0.7

STEEP = 14.0
HEAD = 2.0 ** (-125.0 / 64.0)


def gained(w_ref, a_ref, gain):
    fresh = keep_rate * a_ref[...] + (1.0 - keep_rate) * w_ref[...]
    return fresh * gain


def tall_gain(gain_ref, height, width):
    lanes = jnp.broadcast_to(gain_ref[...], (128, height)).T
    return jnp.concatenate([lanes] * (width // 128), axis=1)


def coded(x):
    size = jnp.abs(x)
    m = jnp.max(size, axis=0, keepdims=True)
    v = HEAD + size * (HEAD * STEEP / jnp.maximum(m, 1e-30))
    for _ in range(6):
        v = v * v
    return jnp.where(x < 0, -v, v).astype(jnp.bfloat16), m


def encode_body(*refs, count):
    ins, outs = refs[: 3 * count], refs[3 * count :]
    for i in range(count):
        w_ref, a_ref, g_ref = ins[3 * i : 3 * i + 3]
        gain = tall_gain(g_ref, *w_ref.shape)
        y, m = coded(gained(w_ref, a_ref, gain))
        outs[2 * i][...] = y
        outs[2 * i + 1][0] = m


def encode(chunks, gain_halves, block):
    w0 = chunks[0][0]
    half_rows, columns = w0.shape[0] // 2, w0.shape[1]
    operands, in_specs, out_shape, out_specs = [], [], [], []
    for w, avg, half in chunks:
        operands += [w, avg, gain_halves[half]]
        tile = pl.BlockSpec((half_rows, block), lambda j, half=half: (half, j))
        in_specs += [tile, tile, pl.BlockSpec((1, half_rows), lambda j: (0, 0))]
        out_shape += [
            jax.ShapeDtypeStruct((half_rows, columns), jnp.bfloat16),
            jax.ShapeDtypeStruct((1, 1, columns), jnp.float32),
        ]
        out_specs += [
            pl.BlockSpec((half_rows, block), lambda j: (0, j)),
            pl.BlockSpec((1, 1, block), lambda j: (0, 0, j)),
        ]
    got = pl.pallas_call(
        functools.partial(encode_body, count=len(chunks)),
        grid=(columns // block,),
        in_specs=in_specs,
        out_specs=out_specs,
        out_shape=out_shape,
        name="encode",
    )(*operands)
    return got[0::2], got[1::2]


def own_body(where_ref, wg_ref, ag_ref, wu_ref, au_ref, g_ref, f_ref, og_ref, ou_ref):
    del where_ref
    gain = tall_gain(g_ref, *wg_ref.shape)
    og_ref[...] = (gained(wg_ref, ag_ref, gain) / f_ref[0:1, :]).astype(jnp.bfloat16)
    ou_ref[...] = (gained(wu_ref, au_ref, gain) / f_ref[1:2, :]).astype(jnp.bfloat16)


def own_share(shard, shards, w_gate, avg_gate, w_up, avg_up, gain, factors, block):
    rows, columns = w_gate.shape
    tile = pl.BlockSpec((rows, block), lambda j, at: (0, j))
    landed = pl.BlockSpec((rows, block), lambda j, at: (at[0], j))
    out = jax.ShapeDtypeStruct((rows * shards, columns), jnp.bfloat16)
    return pl.pallas_call(
        own_body,
        grid_spec=pltpu.PrefetchScalarGridSpec(
            num_scalar_prefetch=1,
            grid=(columns // block,),
            in_specs=[tile] * 4
            + [
                pl.BlockSpec((1, rows), lambda j, at: (0, 0)),
                pl.BlockSpec((2, block), lambda j, at: (0, j)),
            ],
            out_specs=[landed, landed],
        ),
        out_shape=[out, out],
        name="own_share",
    )(jnp.reshape(shard, (1,)), w_gate, avg_gate, w_up, avg_up, gain, factors)


def decode_body(where_ref, y_ref, r_ref, whole_ref, out_ref):
    del where_ref, whole_ref
    y = y_ref[...].astype(jnp.float32)
    v = jnp.exp2(jnp.log2(jnp.abs(y)) * (1.0 / 64.0))
    r = r_ref[0]
    x = v * (r * (1.0 / (STEEP * HEAD))) - r * (1.0 / STEEP)
    out_ref[...] = jnp.where(y < 0, -x, x).astype(jnp.bfloat16)


def decode(whole, chunk, ratios, shard, entry, half, block):
    half_rows, columns = chunk.shape
    where = jnp.stack([2 * shard + half, entry]).astype(jnp.int32)
    return pl.pallas_call(
        decode_body,
        grid_spec=pltpu.PrefetchScalarGridSpec(
            num_scalar_prefetch=1,
            grid=(columns // block,),
            in_specs=[
                pl.BlockSpec((half_rows, block), lambda j, at: (0, j)),
                pl.BlockSpec((1, 1, block), lambda j, at: (at[1], 0, j)),
                pl.BlockSpec(memory_space=pl.ANY),
            ],
            out_specs=pl.BlockSpec((half_rows, block), lambda j, at: (at[0], j)),
        ),
        out_shape=jax.ShapeDtypeStruct(whole.shape, whole.dtype),
        input_output_aliases={3: 0},
        name="decode",
    )(where, chunk, ratios, whole)


def after(value, *tokens):
    return lax.optimization_barrier((value, *tokens))[0]


def local_plane(w_gate, avg_gate, w_up, avg_up, norm_gain):
    rows, columns = w_gate.shape
    block = min(columns, 512)
    half_rows = rows // 2
    me = lax.axis_index("rows")
    place = me // 2
    outer = (place == 0) | (place == 3)
    halves = [norm_gain[:half_rows].reshape(1, half_rows), norm_gain[half_rows:].reshape(1, half_rows)]

    def hop(value, pairs):
        both = [(2 * a + side, 2 * b + side) for a, b in pairs for side in (0, 1)]
        return lax.ppermute(value, "rows", both)

    across = lambda value: lax.ppermute(value, "rows", [(i, i ^ 1) for i in range(8)])
    buddies = lambda value: hop(value, [(0, 1), (1, 0), (2, 3), (3, 2)])
    outward = lambda value: hop(value, [(1, 0), (2, 3)])
    middle = lambda value: hop(value, [(1, 2), (2, 1)])
    skip = lambda value: hop(value, [(0, 2), (2, 0), (1, 3), (3, 1)])

    first, first_max = encode([(w_gate, avg_gate, 0)], halves, block)
    rest, rest_max = encode([(w_up, avg_up, 0), (w_gate, avg_gate, 1), (w_up, avg_up, 1)], halves, block)
    own = [first[0], *rest]
    maxima = jnp.concatenate([first_max[0], *rest_max], axis=0)

    X, B, M, O, V, F = {}, {}, {}, {}, {}, {}
    table = [maxima]
    factors = ratios = None
    wholes = [None, None]
    waiting = []
    own_gain = norm_gain.reshape(1, rows)

    near = jnp.where(place < 2, 2, 1) * 2 + me % 2
    far = jnp.where(place < 2, 3, 0) * 2 + me % 2

    def arrived(k):
        got = [X[k]]
        if k < 4:
            got += [B[k], M[k]]
            waiting.append((X[k], me ^ 1, k))
            waiting.append((B[k], me ^ 2, k))
        elif k < 8:
            got += [O[k], M[k]]
        elif k < 12:
            got += [O[k]]
        else:
            got += [F[k - 12]]
            waiting.append((F[k - 12], me ^ 3, k - 12))
        if 4 <= k < 6:
            waiting.append((X[k], me ^ 3, k - 2))
        if 6 <= k < 10:
            waiting.append((X[k], near ^ 1, k - 6))
        if 10 <= k:
            waiting.append((X[k], far ^ 1, k - 10))
        if 4 <= k < 12:
            j = k - 4
            V[j] = jnp.where(outer, O[k], M[j])
            waiting.append((V[j], near if j < 4 else far, j % 4))
        return got

    def send(k, *tokens):
        tie = lambda value: after(value, *tokens) if tokens else value
        if k < 4:
            X[k] = across(tie(own[k]))
        elif k < 6:
            X[k] = across(tie(B[k - 2]))
        elif k < 14:
            X[k] = across(tie(V[k - 6]))
        if k < 4:
            B[k] = buddies(tie(own[k]))
            M[k] = middle(tie(own[k]))
        elif k < 12:
            O[k] = outward(tie(M[k - 4]))
            if k < 8:
                M[k] = middle(tie(B[k - 4]))
        elif k < 14:
            F[k - 12] = buddies(tie(X[k - 12]))

    def settle(count):
        for _ in range(min(count, len(waiting))):
            chunk, shard, c = waiting.pop(0)
            t = c % 2
            wholes[t] = decode(wholes[t], chunk, ratios, shard, (shard ^ me) * 4 + c, c // 2, block)

    send(0)
    table.append(buddies(maxima))
    send(1)
    for k in range(14):
        got = arrived(k)
        if k + 2 < 14:
            send(k + 2, *got)
        if k == 1:
            table.append(skip(after(jnp.concatenate(table, axis=0), *got)))
        if k == 3:
            table.append(across(after(jnp.concatenate(table, axis=0), *got)))
        if k == 5:
            every = jnp.concatenate(table, axis=0).reshape(2, 4, 4, columns)
            every = jnp.swapaxes(every, 0, 1).reshape(8, 4, columns)
            most = jnp.max(every, axis=0)
            factors = jnp.maximum(most[:2], most[2:])
            ratios = (every / jnp.concatenate([factors, factors], axis=0)).reshape(32, 1, columns)
            wholes = list(own_share(me, 8, w_gate, avg_gate, w_up, avg_up, own_gain, factors, block))
        if k >= 6:
            settle(4 if k < 11 else 3)
    settle(len(waiting))
    return (*wholes, factors[0], factors[1])


def local_any(w_gate, avg_gate, w_up, avg_up, norm_gain):
    fresh_gained_gate = (keep_rate * avg_gate + (1.0 - keep_rate) * w_gate) * norm_gain[:, None]
    fresh_gained_up = (keep_rate * avg_up + (1.0 - keep_rate) * w_up) * norm_gain[:, None]
    factor_gate, factor_up = lax.pmax(
        (jnp.max(jnp.abs(fresh_gained_gate), axis=0), jnp.max(jnp.abs(fresh_gained_up), axis=0)),
        "rows",
    )
    serve_gate = lax.all_gather((fresh_gained_gate / factor_gate).astype(jnp.bfloat16), "rows", axis=0, tiled=True)
    serve_up = lax.all_gather((fresh_gained_up / factor_up).astype(jnp.bfloat16), "rows", axis=0, tiled=True)
    return serve_gate, serve_up, factor_gate, factor_up


def solution(mesh):
    local = local_plane if mesh.shape["rows"] == 8 else local_any
    return jax.shard_map(
        local,
        mesh=mesh,
        in_specs=(P("rows", "width"),) * 4 + (P("rows"),),
        out_specs=(P(None, "width"), P(None, "width"), P("width"), P("width")),
        check_vma=False,
    )
```

```python
import functools

import jax
import jax.numpy as jnp
from jax import lax
from jax.experimental import pallas as pl
from jax.experimental.pallas import tpu as pltpu
from jax.sharding import PartitionSpec as P


keep_rate = 0.7

SPAN = 250.0


def gained(w_ref, a_ref, gain):
    fresh = keep_rate * a_ref[...] + (1.0 - keep_rate) * w_ref[...]
    return fresh * gain


def tall_gain(gain_ref, width):
    rows = gain_ref.shape[0]
    lanes = jnp.broadcast_to(gain_ref[...].reshape(1, rows), (128, rows)).T
    return jnp.concatenate([lanes] * (width // 128), axis=1)


def coded(x):
    size = jnp.abs(x)
    m = jnp.max(size, axis=0, keepdims=True)
    y = jnp.exp2(size * (SPAN / jnp.maximum(m, 1e-30)) - SPAN / 2)
    return jnp.where(x < 0, -y, y).astype(jnp.bfloat16), m


def encode_body(gain_ref, *refs, picks):
    ins, outs = refs[: 2 * len(picks)], refs[2 * len(picks) :]
    half_rows, width = ins[0].shape
    tall = tall_gain(gain_ref, width)
    for i, half in enumerate(picks):
        gain = tall[half * half_rows : (half + 1) * half_rows]
        y, m = coded(gained(ins[2 * i], ins[2 * i + 1], gain))
        outs[2 * i][...] = y
        outs[2 * i + 1][0] = m


def encode(chunks, gain, block):
    half_rows, columns = chunks[0][0].shape[0] // 2, chunks[0][0].shape[1]
    operands, in_specs, out_shape, out_specs = [gain], [pl.BlockSpec(gain.shape, lambda j: (0,))], [], []
    for w, avg, half in chunks:
        operands += [w, avg]
        in_specs += [pl.BlockSpec((half_rows, block), lambda j, half=half: (half, j))] * 2
        out_shape += [
            jax.ShapeDtypeStruct((half_rows, columns), jnp.bfloat16),
            jax.ShapeDtypeStruct((1, 1, columns), jnp.float32),
        ]
        out_specs += [
            pl.BlockSpec((half_rows, block), lambda j: (0, j)),
            pl.BlockSpec((1, 1, block), lambda j: (0, 0, j)),
        ]
    got = pl.pallas_call(
        functools.partial(encode_body, picks=[half for _, _, half in chunks]),
        grid=(columns // block,),
        in_specs=in_specs,
        out_specs=out_specs,
        out_shape=out_shape,
        name="encode",
    )(*operands)
    return got[0::2], got[1::2]


def own_body(me_ref, wg_ref, ag_ref, wu_ref, au_ref, g_ref, f_ref, og_ref, ou_ref, token_ref):
    del me_ref
    gain = tall_gain(g_ref, wg_ref.shape[1])
    og_ref[...] = (gained(wg_ref, ag_ref, gain) / f_ref[0:1, :]).astype(jnp.bfloat16)
    ou_ref[...] = (gained(wu_ref, au_ref, gain) / f_ref[1:2, :]).astype(jnp.bfloat16)
    token_ref[...] = jnp.zeros_like(token_ref)


def own_share(me, shards, w_gate, avg_gate, w_up, avg_up, gain, factors, block):
    rows, columns = w_gate.shape
    tile = pl.BlockSpec((rows, block), lambda j, me: (0, j))
    landed = pl.BlockSpec((rows, block), lambda j, me: (me[0], j))
    out = jax.ShapeDtypeStruct((rows * shards, columns), jnp.bfloat16)
    return pl.pallas_call(
        own_body,
        grid_spec=pltpu.PrefetchScalarGridSpec(
            num_scalar_prefetch=1,
            grid=(columns // block,),
            in_specs=[tile] * 4
            + [
                pl.BlockSpec(gain.shape, lambda j, me: (0,)),
                pl.BlockSpec((2, block), lambda j, me: (0, j)),
            ],
            out_specs=[landed, landed, pl.BlockSpec((8, 128), lambda j, me: (0, 0))],
        ),
        out_shape=[out, out, jax.ShapeDtypeStruct((8, 128), jnp.float32)],
        name="own_share",
    )(me, w_gate, avg_gate, w_up, avg_up, gain, factors)


def ratios_body(*refs):
    tables, (ratio_ref, factor_ref) = refs[:-2], refs[-2:]
    order = [0, 2, 4, 6, 1, 3, 5, 7]
    rows = [ref[i] for ref in tables for i in range(ref.shape[0])]
    for t in range(2):
        mine = [rows[4 * place + c] for place in range(8) for c in (t, t + 2)]
        factor = functools.reduce(jnp.maximum, mine)
        factor_ref[t : t + 1, :] = factor
        for place, shard in enumerate(order):
            for c in (t, t + 2):
                ratio_ref[4 * shard + c] = rows[4 * place + c] / factor


def ratios_of(tables):
    columns = tables[0].shape[-1]
    return pl.pallas_call(
        ratios_body,
        out_shape=[
            jax.ShapeDtypeStruct((32, 1, columns), jnp.float32),
            jax.ShapeDtypeStruct((2, columns), jnp.float32),
        ],
        name="ratios",
    )(*tables)


def decode_body(me_ref, y_ref, r_ref, whole_ref, out_ref, token_ref):
    del me_ref, whole_ref
    y = y_ref[...].astype(jnp.float32)
    r = r_ref[0]
    x = jnp.log2(jnp.abs(y)) * (r * (1.0 / SPAN)) + r * 0.5
    out_ref[...] = jnp.where(y < 0, -x, x).astype(jnp.bfloat16)
    token_ref[...] = jnp.zeros_like(token_ref)


def decode(whole, chunk, ratios, me, shard_of, c, block):
    half_rows, columns = chunk.shape
    return pl.pallas_call(
        decode_body,
        grid_spec=pltpu.PrefetchScalarGridSpec(
            num_scalar_prefetch=1,
            grid=(columns // block,),
            in_specs=[
                pl.BlockSpec((half_rows, block), lambda j, me: (0, j)),
                pl.BlockSpec((1, 1, block), lambda j, me: ((shard_of(me[0]) ^ me[0]) * 4 + c, 0, j)),
                pl.BlockSpec(memory_space=pl.ANY),
            ],
            out_specs=[
                pl.BlockSpec((half_rows, block), lambda j, me: (2 * shard_of(me[0]) + c // 2, j)),
                pl.BlockSpec((8, 128), lambda j, me: (0, 0)),
            ],
        ),
        out_shape=[
            jax.ShapeDtypeStruct(whole.shape, whole.dtype),
            jax.ShapeDtypeStruct((8, 128), jnp.float32),
        ],
        input_output_aliases={3: 0},
        name="decode",
    )(me, chunk, ratios, whole)


def after(value, *tokens):
    return lax.optimization_barrier((value, *tokens))[0]


def across_of(me):
    return me ^ 1


def buddy_of(me):
    return me ^ 2


def diagonal_of(me):
    return me ^ 3


def near_of(me):
    return jnp.where(me < 4, 4, 2) + (me & 1)


def far_of(me):
    return jnp.where(me < 4, 6, 0) + (me & 1)


def near_across_of(me):
    return near_of(me) ^ 1


def far_across_of(me):
    return far_of(me) ^ 1


def local_plane(w_gate, avg_gate, w_up, avg_up, norm_gain):
    block = min(w_gate.shape[1], 1024)
    index = lax.axis_index("rows")
    outer = (index < 2) | (index >= 6)
    me = jnp.reshape(index, (1,)).astype(jnp.int32)

    def hop(value, pairs):
        both = [(2 * a + side, 2 * b + side) for a, b in pairs for side in (0, 1)]
        return lax.ppermute(value, "rows", both)

    across = lambda value: lax.ppermute(value, "rows", [(i, i ^ 1) for i in range(8)])
    buddies = lambda value: hop(value, [(0, 1), (1, 0), (2, 3), (3, 2)])
    outward = lambda value: hop(value, [(1, 0), (2, 3)])
    middle = lambda value: hop(value, [(1, 2), (2, 1)])
    skip = lambda value: hop(value, [(0, 2), (2, 0), (1, 3), (3, 1)])

    first, first_max = encode([(w_gate, avg_gate, 0)], norm_gain, block)
    with jax.named_scope("rest"):
        rest, rest_max = encode([(w_up, avg_up, 0), (w_gate, avg_gate, 1), (w_up, avg_up, 1)], norm_gain, block // 2)
    own = [first[0], *rest]
    maxima = jnp.concatenate([first_max[0], *rest_max], axis=0)

    X, B, M, O, V, F = {}, {}, {}, {}, {}, {}
    tables = [maxima]
    factors = ratios = None
    wholes, tokens, waiting = [None, None], [], []

    def arrived(k):
        got = [X[k]]
        if k < 4:
            got += [B[k], M[k]]
            waiting.extend([(X[k], across_of, k), (B[k], buddy_of, k)])
        elif k < 8:
            got += [O[k], M[k]]
        elif k < 12:
            got += [O[k]]
        else:
            got += [F[k - 12]]
            waiting.append((F[k - 12], diagonal_of, k - 12))
        if 4 <= k < 6:
            waiting.append((X[k], diagonal_of, k - 2))
        if 6 <= k < 10:
            waiting.append((X[k], near_across_of, k - 6))
        if 10 <= k:
            waiting.append((X[k], far_across_of, k - 10))
        if 4 <= k < 12:
            j = k - 4
            V[j] = jnp.where(outer, O[k], M[j])
            waiting.append((V[j], near_of if j < 4 else far_of, j % 4))
        return got

    def send(k, *ties):
        tie = lambda value: after(value, *ties) if ties else value
        with jax.named_scope(f"across{k}"):
            if k < 4:
                X[k] = across(tie(own[k]))
            elif k < 6:
                X[k] = across(tie(B[k - 2]))
            else:
                X[k] = across(tie(V[k - 6]))
        with jax.named_scope(f"along{k}"):
            if k < 4:
                B[k] = buddies(tie(own[k]))
            elif k < 12:
                O[k] = outward(tie(M[k - 4]))
            else:
                F[k - 12] = buddies(tie(X[k - 12]))
        with jax.named_scope(f"middle{k}"):
            if k < 4:
                M[k] = middle(tie(own[k]))
            elif k < 8:
                M[k] = middle(tie(B[k - 4]))

    def settle(count):
        done = []
        for _ in range(min(count, len(waiting))):
            chunk, shard_of, c = waiting.pop(0)
            wholes[c % 2], token = decode(wholes[c % 2], chunk, ratios, me, shard_of, c, block)
            done.append(token)
        return done

    send(0)
    with jax.named_scope("maxima0"):
        tables.append(buddies(maxima))
    send(1)
    for k in range(14):
        got = arrived(k)
        if k == 0:
            got.append(tables[1])
            with jax.named_scope("maxima1"):
                tables.append(skip(after(jnp.concatenate(tables, axis=0), *got)))
        if k == 1:
            got.append(tables[2])
            with jax.named_scope("maxima2"):
                tables.append(across(after(jnp.concatenate(tables, axis=0), *got)))
        if k == 2:
            got.append(tables[3])
            ratios, factors = ratios_of(tables)
        if k + 2 < 14:
            send(k + 2, *got, *tokens)
        if k == 2:
            *wholes, token = own_share(me, 8, w_gate, avg_gate, w_up, avg_up, norm_gain, factors, block // 2)
            tokens = [token]
        if k >= 3:
            tokens = settle(3)
    settle(len(waiting))
    return (*wholes, factors[0], factors[1])


def local_any(w_gate, avg_gate, w_up, avg_up, norm_gain):
    fresh_gained_gate = (keep_rate * avg_gate + (1.0 - keep_rate) * w_gate) * norm_gain[:, None]
    fresh_gained_up = (keep_rate * avg_up + (1.0 - keep_rate) * w_up) * norm_gain[:, None]
    factor_gate, factor_up = lax.pmax(
        (jnp.max(jnp.abs(fresh_gained_gate), axis=0), jnp.max(jnp.abs(fresh_gained_up), axis=0)),
        "rows",
    )
    serve_gate = lax.all_gather((fresh_gained_gate / factor_gate).astype(jnp.bfloat16), "rows", axis=0, tiled=True)
    serve_up = lax.all_gather((fresh_gained_up / factor_up).astype(jnp.bfloat16), "rows", axis=0, tiled=True)
    return serve_gate, serve_up, factor_gate, factor_up


def solution(mesh):
    local = local_plane if mesh.shape["rows"] == 8 else local_any
    return jax.shard_map(
        local,
        mesh=mesh,
        in_specs=(P("rows", "width"),) * 4 + (P("rows"),),
        out_specs=(P(None, "width"), P(None, "width"), P("width"), P("width")),
        check_vma=False,
    )
```

```python
import functools

import jax
import jax.numpy as jnp
from jax import lax
from jax.experimental import pallas as pl
from jax.experimental.pallas import tpu as pltpu
from jax.sharding import PartitionSpec as P


keep_rate = 0.7

SPAN = 250.0


def gained(w_ref, a_ref, gain):
    fresh = keep_rate * a_ref[...] + (1.0 - keep_rate) * w_ref[...]
    return fresh * gain


def tall_gain(gain_ref, width):
    rows = gain_ref.shape[0]
    lanes = jnp.broadcast_to(gain_ref[...].reshape(1, rows), (128, rows)).T
    return jnp.concatenate([lanes] * (width // 128), axis=1)


def coded(x):
    size = jnp.abs(x)
    m = jnp.max(size, axis=0, keepdims=True)
    y = jnp.exp2(size * (SPAN / jnp.maximum(m, 1e-30)) - SPAN / 2)
    return jnp.where(x < 0, -y, y).astype(jnp.bfloat16), m


def encode_body(gain_ref, *refs, picks, earlier):
    count = len(picks)
    ins, outs = refs[: 2 * count], refs[2 * count + earlier :]
    half_rows, width = ins[0].shape
    tall = tall_gain(gain_ref, width)
    for i, half in enumerate(picks):
        gain = tall[half * half_rows : (half + 1) * half_rows]
        y, m = coded(gained(ins[2 * i], ins[2 * i + 1], gain))
        outs[i][...] = y
        outs[count][earlier + i] = m
    if earlier:
        outs[count][0] = refs[2 * count][0]


def encode(chunks, gain, block, maxima=None):
    half_rows, columns = chunks[0][0].shape[0] // 2, chunks[0][0].shape[1]
    operands, in_specs, out_shape, out_specs = [gain], [pl.BlockSpec(gain.shape, lambda j: (0,))], [], []
    earlier = 0 if maxima is None else 1
    for w, avg, half in chunks:
        operands += [w, avg]
        in_specs += [pl.BlockSpec((half_rows, block), lambda j, half=half: (half, j))] * 2
        out_shape.append(jax.ShapeDtypeStruct((half_rows, columns), jnp.bfloat16))
        out_specs.append(pl.BlockSpec((half_rows, block), lambda j: (0, j)))
    if earlier:
        operands.append(maxima)
        in_specs.append(pl.BlockSpec((1, 1, block), lambda j: (0, 0, j)))
    count = earlier + len(chunks)
    return pl.pallas_call(
        functools.partial(encode_body, picks=[half for _, _, half in chunks], earlier=earlier),
        grid=(columns // block,),
        in_specs=in_specs,
        out_specs=out_specs + [pl.BlockSpec((count, 1, block), lambda j: (0, 0, j))],
        out_shape=out_shape + [jax.ShapeDtypeStruct((count, 1, columns), jnp.float32)],
        name="encode",
    )(*operands)


def own_body(me_ref, wg_ref, ag_ref, wu_ref, au_ref, g_ref, f_ref, og_ref, ou_ref, token_ref):
    del me_ref
    gain = tall_gain(g_ref, wg_ref.shape[1])
    og_ref[...] = (gained(wg_ref, ag_ref, gain) / f_ref[0:1, :]).astype(jnp.bfloat16)
    ou_ref[...] = (gained(wu_ref, au_ref, gain) / f_ref[1:2, :]).astype(jnp.bfloat16)
    token_ref[...] = jnp.zeros_like(token_ref)


def own_share(me, shards, w_gate, avg_gate, w_up, avg_up, gain, factors, block):
    rows, columns = w_gate.shape
    tile = pl.BlockSpec((rows, block), lambda j, me: (0, j))
    landed = pl.BlockSpec((rows, block), lambda j, me: (me[0], j))
    out = jax.ShapeDtypeStruct((rows * shards, columns), jnp.bfloat16)
    return pl.pallas_call(
        own_body,
        grid_spec=pltpu.PrefetchScalarGridSpec(
            num_scalar_prefetch=1,
            grid=(columns // block,),
            in_specs=[tile] * 4
            + [
                pl.BlockSpec(gain.shape, lambda j, me: (0,)),
                pl.BlockSpec((2, block), lambda j, me: (0, j)),
            ],
            out_specs=[landed, landed, pl.BlockSpec((8, 128), lambda j, me: (0, 0))],
        ),
        out_shape=[out, out, jax.ShapeDtypeStruct((8, 128), jnp.float32)],
        name="own_share",
    )(me, w_gate, avg_gate, w_up, avg_up, gain, factors)


def ratios_body(*refs):
    tables, (ratio_ref, factor_ref) = refs[:-2], refs[-2:]
    order = [0, 2, 4, 6, 1, 3, 5, 7]
    rows = [ref[i] for ref in tables for i in range(ref.shape[0])]
    for t in range(2):
        mine = [rows[4 * place + c] for place in range(8) for c in (t, t + 2)]
        factor = functools.reduce(jnp.maximum, mine)
        factor_ref[t : t + 1, :] = factor
        for place, shard in enumerate(order):
            for c in (t, t + 2):
                ratio_ref[4 * shard + c] = rows[4 * place + c] / factor


def ratios_of(tables):
    columns = tables[0].shape[-1]
    return pl.pallas_call(
        ratios_body,
        out_shape=[
            jax.ShapeDtypeStruct((32, 1, columns), jnp.float32),
            jax.ShapeDtypeStruct((2, columns), jnp.float32),
        ],
        name="ratios",
    )(*tables)


def decoded(y, ratio):
    y = y.astype(jnp.float32)
    x = jnp.log2(jnp.abs(y)) * (ratio * (1.0 / SPAN)) + ratio * 0.5
    return jnp.where(y < 0, -x, x).astype(jnp.bfloat16)


def decode_body(me_ref, y_ref, r_ref, whole_ref, out_ref, token_ref):
    del me_ref, whole_ref
    out_ref[...] = decoded(y_ref[...], r_ref[0])
    token_ref[...] = jnp.zeros_like(token_ref)


def decode(whole, chunk, ratios, me, shard_of, c, block):
    half_rows, columns = chunk.shape
    return pl.pallas_call(
        decode_body,
        grid_spec=pltpu.PrefetchScalarGridSpec(
            num_scalar_prefetch=1,
            grid=(columns // block,),
            in_specs=[
                pl.BlockSpec((half_rows, block), lambda j, me: (0, j)),
                pl.BlockSpec((1, 1, block), lambda j, me: ((shard_of(me[0]) ^ me[0]) * 4 + c, 0, j)),
                pl.BlockSpec(memory_space=pl.ANY),
            ],
            out_specs=[
                pl.BlockSpec((half_rows, block), lambda j, me: (2 * shard_of(me[0]) + c // 2, j)),
                pl.BlockSpec((8, 128), lambda j, me: (0, 0)),
            ],
        ),
        out_shape=[
            jax.ShapeDtypeStruct(whole.shape, whole.dtype),
            jax.ShapeDtypeStruct((8, 128), jnp.float32),
        ],
        input_output_aliases={3: 0},
        name="decode",
    )(me, chunk, ratios, whole)


def last_body(me_ref, y0_ref, y1_ref, r0_ref, r1_ref, whole_ref, out_ref, buffer, sems, *, starts_of, pieces):
    del whole_ref
    rows = y0_ref.shape[0] // pieces
    copies = []
    for i, (y_ref, r_ref) in enumerate(((y0_ref, r0_ref), (y1_ref, r1_ref))):
        start = starts_of[i](me_ref[0]) * y_ref.shape[0]
        for p in range(pieces):
            part = pl.ds(p * rows, rows)
            buffer[i, part] = decoded(y_ref[part], r_ref[0])
            copies.append(
                pltpu.make_async_copy(buffer.at[i, part], out_ref.at[pl.ds(start + p * rows, rows)], sems.at[i, p])
            )
            copies[-1].start()
    for copy in copies:
        copy.wait()


def decode_last(whole, chunks, ratios, me, shards_of, cs, pieces=4):
    half_rows, columns = chunks[0].shape
    kept = pl.BlockSpec(memory_space=pltpu.VMEM)
    ratio = lambda shard_of, c: pl.BlockSpec(
        (1, 1, columns), lambda j, me: ((shard_of(me[0]) ^ me[0]) * 4 + c, 0, 0)
    )
    starts_of = [lambda me, at=at, c=c: 2 * at(me) + c // 2 for at, c in zip(shards_of, cs)]
    return pl.pallas_call(
        functools.partial(last_body, starts_of=starts_of, pieces=pieces),
        grid_spec=pltpu.PrefetchScalarGridSpec(
            num_scalar_prefetch=1,
            grid=(1,),
            in_specs=[kept, kept, *map(ratio, shards_of, cs), pl.BlockSpec(memory_space=pl.ANY)],
            out_specs=pl.BlockSpec(memory_space=pl.ANY),
            scratch_shapes=[
                pltpu.VMEM((2, half_rows, columns), whole.dtype),
                pltpu.SemaphoreType.DMA((2, pieces)),
            ],
        ),
        out_shape=jax.ShapeDtypeStruct(whole.shape, whole.dtype),
        input_output_aliases={5: 0},
        name="decode_last",
    )(me, *chunks, ratios, ratios, whole)


def after(value, *tokens):
    return lax.optimization_barrier((value, *tokens))[0]


def across_of(me):
    return me ^ 1


def buddy_of(me):
    return me ^ 2


def diagonal_of(me):
    return me ^ 3


def near_of(me):
    return jnp.where(me < 4, 4, 2) + (me & 1)


def far_of(me):
    return jnp.where(me < 4, 6, 0) + (me & 1)


def near_across_of(me):
    return near_of(me) ^ 1


def far_across_of(me):
    return far_of(me) ^ 1


def local_plane(w_gate, avg_gate, w_up, avg_up, norm_gain):
    block = min(w_gate.shape[1], 1024)
    index = lax.axis_index("rows")
    outer = (index < 2) | (index >= 6)
    me = jnp.reshape(index, (1,)).astype(jnp.int32)

    def hop(value, pairs):
        both = [(2 * a + side, 2 * b + side) for a, b in pairs for side in (0, 1)]
        return lax.ppermute(value, "rows", both)

    across = lambda value: lax.ppermute(value, "rows", [(i, i ^ 1) for i in range(8)])
    buddies = lambda value: hop(value, [(0, 1), (1, 0), (2, 3), (3, 2)])
    outward = lambda value: hop(value, [(1, 0), (2, 3)])
    middle = lambda value: hop(value, [(1, 2), (2, 1)])
    skip = lambda value: hop(value, [(0, 2), (2, 0), (1, 3), (3, 1)])

    first, maxima = encode([(w_gate, avg_gate, 0)], norm_gain, block)
    others = [(w_up, avg_up, 0), (w_gate, avg_gate, 1), (w_up, avg_up, 1)]
    *rest, maxima = encode(others, norm_gain, block // 2, maxima)
    own = [first, *rest]

    X, B, M, O, V, F = {}, {}, {}, {}, {}, {}
    tables = [maxima]
    factors = ratios = None
    wholes, tokens, waiting = [None, None], [], []

    def arrived(k):
        got = [X[k]]
        if k < 4:
            got += [B[k], M[k]]
            waiting.extend([(X[k], across_of, k), (B[k], buddy_of, k)])
        elif k < 8:
            got += [O[k], M[k]]
        elif k < 12:
            got += [O[k]]
        else:
            got += [F[k - 12]]
            waiting.append((F[k - 12], diagonal_of, k - 12))
        if 4 <= k < 6:
            waiting.append((X[k], diagonal_of, k - 2))
        if 6 <= k < 10:
            waiting.append((X[k], near_across_of, k - 6))
        if 10 <= k:
            waiting.append((X[k], far_across_of, k - 10))
        if 4 <= k < 12:
            j = k - 4
            V[j] = jnp.where(outer, O[k], M[j])
            waiting.append((V[j], near_of if j < 4 else far_of, j % 4))
        return got

    def send(k, *ties):
        tie = lambda value: after(value, *ties) if ties else value
        if k < 4:
            X[k] = across(tie(own[k]))
        elif k < 6:
            X[k] = across(tie(B[k - 2]))
        else:
            X[k] = across(tie(V[k - 6]))
        if k < 4:
            B[k] = buddies(tie(own[k]))
        elif k < 12:
            O[k] = outward(tie(M[k - 4]))
        else:
            F[k - 12] = buddies(tie(X[k - 12]))
        if k < 4:
            M[k] = middle(tie(own[k]))
        elif k < 8:
            M[k] = middle(tie(B[k - 4]))

    def settle(count):
        done = []
        for _ in range(min(count, len(waiting))):
            chunk, shard_of, c = waiting.pop(0)
            wholes[c % 2], token = decode(wholes[c % 2], chunk, ratios, me, shard_of, c, block)
            done.append(token)
        return done

    send(0)
    tables.append(buddies(maxima))
    send(1)
    for k in range(14):
        got = arrived(k)
        if k == 0:
            got.append(tables[1])
            tables.append(skip(after(jnp.concatenate(tables, axis=0), *got)))
        if k == 1:
            got.append(tables[2])
            tables.append(across(after(jnp.concatenate(tables, axis=0), *got)))
        if k == 2:
            got.append(tables[3])
            ratios, factors = ratios_of(tables)
        if k + 2 < 14:
            send(k + 2, *got, *tokens)
        if k == 2:
            *wholes, token = own_share(me, 8, w_gate, avg_gate, w_up, avg_up, norm_gain, factors, block // 2)
            tokens = [token]
        if k >= 3:
            tokens = settle(3 if k < 13 else len(waiting) - 2)
    chunks, shards_of, cs = zip(*waiting)
    t = cs[0] % 2
    wholes[t] = decode_last(wholes[t], chunks, ratios, me, shards_of, cs)
    return (*wholes, factors[0], factors[1])


def local_any(w_gate, avg_gate, w_up, avg_up, norm_gain):
    fresh_gained_gate = (keep_rate * avg_gate + (1.0 - keep_rate) * w_gate) * norm_gain[:, None]
    fresh_gained_up = (keep_rate * avg_up + (1.0 - keep_rate) * w_up) * norm_gain[:, None]
    factor_gate, factor_up = lax.pmax(
        (jnp.max(jnp.abs(fresh_gained_gate), axis=0), jnp.max(jnp.abs(fresh_gained_up), axis=0)),
        "rows",
    )
    serve_gate = lax.all_gather((fresh_gained_gate / factor_gate).astype(jnp.bfloat16), "rows", axis=0, tiled=True)
    serve_up = lax.all_gather((fresh_gained_up / factor_up).astype(jnp.bfloat16), "rows", axis=0, tiled=True)
    return serve_gate, serve_up, factor_gate, factor_up


def solution(mesh):
    plane = mesh.shape["rows"] == 8

    def local(*args):
        return (local_plane if plane else local_any)(*args)

    return jax.shard_map(
        local,
        mesh=mesh,
        in_specs=(P("rows", "width"),) * 4 + (P("rows"),),
        out_specs=(P(None, "width"), P(None, "width"), P("width"), P("width")),
        check_vma=False,
    )
```

```python
import functools

import jax
import jax.numpy as jnp
from jax import lax
from jax.experimental import pallas as pl
from jax.experimental.pallas import tpu as pltpu
from jax.sharding import PartitionSpec as P


keep_rate = 0.7

SPAN = 250.0


KERNEL_VMEM = 14 * 2**20


def near_by(value):
    return pltpu.with_memory_space_constraint(value, pltpu.VMEM)


def stay_out(value):
    return pltpu.with_memory_space_constraint(value, pltpu.HBM)


def gained(w_ref, a_ref, gain):
    fresh = keep_rate * a_ref[...] + (1.0 - keep_rate) * w_ref[...]
    return fresh * gain


def tall_gain(gain_ref, width):
    rows = gain_ref.shape[0]
    lanes = jnp.broadcast_to(gain_ref[...].reshape(1, rows), (128, rows)).T
    return jnp.concatenate([lanes] * (width // 128), axis=1)


def coded(x):
    size = jnp.abs(x)
    m = jnp.max(size, axis=0, keepdims=True)
    y = jnp.exp2(size * (SPAN / jnp.maximum(m, 1e-30)) - SPAN / 2)
    return jnp.where(x < 0, -y, y).astype(jnp.bfloat16), m


def encode_body(gain_ref, *refs, picks, earlier):
    count = len(picks)
    ins, outs = refs[: 2 * count], refs[2 * count + earlier :]
    half_rows, width = ins[0].shape
    tall = tall_gain(gain_ref, width)
    for i, half in enumerate(picks):
        gain = tall[half * half_rows : (half + 1) * half_rows]
        y, m = coded(gained(ins[2 * i], ins[2 * i + 1], gain))
        outs[i][...] = y
        outs[count][earlier + i] = m
    if earlier:
        outs[count][0] = refs[2 * count][0]


def encode(chunks, gain, block, maxima=None):
    half_rows, columns = chunks[0][0].shape[0] // 2, chunks[0][0].shape[1]
    operands, in_specs, out_shape, out_specs = [gain], [pl.BlockSpec(gain.shape, lambda j: (0,))], [], []
    earlier = 0 if maxima is None else 1
    for w, avg, half in chunks:
        operands += [stay_out(w), stay_out(avg)]
        in_specs += [pl.BlockSpec((half_rows, block), lambda j, half=half: (half, j))] * 2
        out_shape.append(jax.ShapeDtypeStruct((half_rows, columns), jnp.bfloat16))
        out_specs.append(pl.BlockSpec((half_rows, block), lambda j: (0, j)))
    if earlier:
        operands.append(maxima)
        in_specs.append(pl.BlockSpec((1, 1, block), lambda j: (0, 0, j)))
    count = earlier + len(chunks)
    return pl.pallas_call(
        functools.partial(encode_body, picks=[half for _, _, half in chunks], earlier=earlier),
        grid=(columns // block,),
        in_specs=in_specs,
        out_specs=out_specs + [pl.BlockSpec((count, 1, block), lambda j: (0, 0, j))],
        out_shape=out_shape + [jax.ShapeDtypeStruct((count, 1, columns), jnp.float32)],
        compiler_params=pltpu.CompilerParams(vmem_limit_bytes=KERNEL_VMEM),
        name="encode",
    )(*operands)


def encode_first_body(g_ref, w_ref, a_ref, y_ref, m_ref, gain_ref, ws, avgs, sems, *, half):
    half_rows, _ = y_ref.shape
    steps, _, width = ws.shape
    copies = []
    gain_copy = pltpu.make_async_copy(g_ref, gain_ref, sems.at[2, 0])
    gain_copy.start()
    for j in range(steps):
        source = (pl.ds(half * half_rows, half_rows), pl.ds(j * width, width))
        pair = [
            pltpu.make_async_copy(ref.at[source], held.at[j], sems.at[i, j])
            for i, (ref, held) in enumerate(((w_ref, ws), (a_ref, avgs)))
        ]
        for copy in pair:
            copy.start()
        copies.append(pair)
    gain_copy.wait()
    gain = tall_gain(gain_ref, width)[half * half_rows : (half + 1) * half_rows]
    for j, pair in enumerate(copies):
        for copy in pair:
            copy.wait()
        part = pl.ds(j * width, width)
        y, m = coded(gained(ws.at[j], avgs.at[j], gain))
        y_ref[:, part] = y
        m_ref[0, :, part] = m


def encode_first(w, avg, gain, half, width):
    half_rows, columns = w.shape[0] // 2, w.shape[1]
    here = pl.BlockSpec(memory_space=pltpu.VMEM)
    there = pl.BlockSpec(memory_space=pl.ANY)
    held = pltpu.VMEM((columns // width, half_rows, width), jnp.float32)
    return pl.pallas_call(
        functools.partial(encode_first_body, half=half),
        in_specs=[there, there, there],
        out_specs=[here, here],
        out_shape=[
            pltpu.VMEM((half_rows, columns), jnp.bfloat16),
            pltpu.VMEM((1, 1, columns), jnp.float32),
        ],
        scratch_shapes=[pltpu.VMEM(gain.shape, gain.dtype), held, held, pltpu.SemaphoreType.DMA((3, columns // width))],
        compiler_params=pltpu.CompilerParams(vmem_limit_bytes=KERNEL_VMEM),
        name="encode_first",
    )(stay_out(gain), stay_out(w), stay_out(avg))


def own_body(me_ref, wg_ref, ag_ref, wu_ref, au_ref, g_ref, f_ref, og_ref, ou_ref, token_ref):
    del me_ref
    gain = tall_gain(g_ref, wg_ref.shape[1])
    og_ref[...] = (gained(wg_ref, ag_ref, gain) / f_ref[0:1, :]).astype(jnp.bfloat16)
    ou_ref[...] = (gained(wu_ref, au_ref, gain) / f_ref[1:2, :]).astype(jnp.bfloat16)
    token_ref[...] = jnp.zeros_like(token_ref)


def own_share(me, shards, w_gate, avg_gate, w_up, avg_up, gain, factors, block):
    rows, columns = w_gate.shape
    tile = pl.BlockSpec((rows, block), lambda j, me: (0, j))
    landed = pl.BlockSpec((rows, block), lambda j, me: (me[0], j))
    out = jax.ShapeDtypeStruct((rows * shards, columns), jnp.bfloat16)
    return pl.pallas_call(
        own_body,
        grid_spec=pltpu.PrefetchScalarGridSpec(
            num_scalar_prefetch=1,
            grid=(columns // block,),
            in_specs=[tile] * 4
            + [
                pl.BlockSpec(gain.shape, lambda j, me: (0,)),
                pl.BlockSpec((2, block), lambda j, me: (0, j)),
            ],
            out_specs=[landed, landed, pl.BlockSpec((8, 128), lambda j, me: (0, 0))],
        ),
        out_shape=[out, out, jax.ShapeDtypeStruct((8, 128), jnp.float32)],
        compiler_params=pltpu.CompilerParams(vmem_limit_bytes=KERNEL_VMEM),
        name="own_share",
    )(me, *map(stay_out, (w_gate, avg_gate, w_up, avg_up)), gain, factors)


def ratios_body(*refs):
    tables, (ratio_ref, factor_ref) = refs[:-2], refs[-2:]
    order = [0, 2, 4, 6, 1, 3, 5, 7]
    rows = [ref[i] for ref in tables for i in range(ref.shape[0])]
    for t in range(2):
        mine = [rows[4 * place + c] for place in range(8) for c in (t, t + 2)]
        factor = functools.reduce(jnp.maximum, mine)
        factor_ref[t : t + 1, :] = factor
        for place, shard in enumerate(order):
            for c in (t, t + 2):
                ratio_ref[4 * shard + c] = rows[4 * place + c] / factor


def ratios_of(tables):
    columns = tables[0].shape[-1]
    return pl.pallas_call(
        ratios_body,
        out_shape=[
            pltpu.VMEM((32, 1, columns), jnp.float32),
            jax.ShapeDtypeStruct((2, columns), jnp.float32),
        ],
        compiler_params=pltpu.CompilerParams(vmem_limit_bytes=KERNEL_VMEM),
        name="ratios",
    )(*map(near_by, tables))


def decoded(y, ratio):
    y = y.astype(jnp.float32)
    x = jnp.log2(jnp.abs(y)) * (ratio * (1.0 / SPAN)) + ratio * 0.5
    return jnp.where(y < 0, -x, x).astype(jnp.bfloat16)


def decode_body(me_ref, r_ref, *refs, places, pieces):
    count = len(places)
    chunks, (out_ref, token_ref, buffer, sems) = refs[:count], refs[count + 1 :]
    rows = chunks[0].shape[0] // pieces
    me = me_ref[0]
    copies = []
    for i, (shard_of, c) in enumerate(places):
        shard = shard_of(me)
        ratio = r_ref[(shard ^ me) * 4 + c]
        start = (2 * shard + c // 2) * chunks[0].shape[0]
        for p in range(pieces):
            part = pl.ds(p * rows, rows)
            buffer[i, part] = decoded(chunks[i][part], ratio)
            copies.append(
                pltpu.make_async_copy(buffer.at[i, part], out_ref.at[pl.ds(start + p * rows, rows)], sems.at[i, p])
            )
            copies[-1].start()
    token_ref[...] = jnp.zeros_like(token_ref)
    for copy in copies:
        copy.wait()


def decode(whole, chunks, ratios, me, places, pieces=4):
    here = pl.BlockSpec(memory_space=pltpu.VMEM)
    there = pl.BlockSpec(memory_space=pl.ANY)
    return pl.pallas_call(
        functools.partial(decode_body, places=places, pieces=pieces),
        in_specs=[pl.BlockSpec(memory_space=pltpu.SMEM), here] + [here] * len(chunks) + [there],
        out_specs=[there, here],
        out_shape=[
            jax.ShapeDtypeStruct(whole.shape, whole.dtype),
            pltpu.VMEM((8, 128), jnp.float32),
        ],
        scratch_shapes=[
            pltpu.VMEM((len(chunks), *chunks[0].shape), whole.dtype),
            pltpu.SemaphoreType.DMA((len(chunks), pieces)),
        ],
        input_output_aliases={2 + len(chunks): 0},
        compiler_params=pltpu.CompilerParams(vmem_limit_bytes=KERNEL_VMEM),
        name="decode",
    )(me, near_by(ratios), *map(near_by, chunks), whole)


def after(value, *tokens):
    return lax.optimization_barrier((value, *tokens))[0]


def across_of(me):
    return me ^ 1


def buddy_of(me):
    return me ^ 2


def diagonal_of(me):
    return me ^ 3


def near_of(me):
    return jnp.where(me < 4, 4, 2) + (me & 1)


def far_of(me):
    return jnp.where(me < 4, 6, 0) + (me & 1)


def near_across_of(me):
    return near_of(me) ^ 1


def far_across_of(me):
    return far_of(me) ^ 1


def local_plane(w_gate, avg_gate, w_up, avg_up, norm_gain):
    block = min(w_gate.shape[1], 1024)
    index = lax.axis_index("rows")
    outer = (index < 2) | (index >= 6)
    me = jnp.reshape(index, (1,)).astype(jnp.int32)

    def hop(value, pairs):
        both = [(2 * a + side, 2 * b + side) for a, b in pairs for side in (0, 1)]
        return lax.ppermute(value, "rows", both)

    across = lambda value: lax.ppermute(value, "rows", [(i, i ^ 1) for i in range(8)])
    buddies = lambda value: hop(value, [(0, 1), (1, 0), (2, 3), (3, 2)])
    outward = lambda value: hop(value, [(1, 0), (2, 3)])
    middle = lambda value: hop(value, [(1, 2), (2, 1)])
    skip = lambda value: hop(value, [(0, 2), (2, 0), (1, 3), (3, 1)])

    first, maxima = encode_first(w_gate, avg_gate, norm_gain, 0, block // 4)
    others = [(w_up, avg_up, 0), (w_gate, avg_gate, 1), (w_up, avg_up, 1)]
    *rest, maxima = encode(others, norm_gain, block // 2, near_by(maxima))
    own = [first, *rest]

    X, B, M, O, V, F = {}, {}, {}, {}, {}, {}
    tables = [maxima]
    factors = ratios = None
    wholes, tokens, waiting = [None, None], [], []

    def arrived(k):
        got = [X[k]]
        if k < 4:
            got += [B[k], M[k]]
            waiting.extend([(X[k], across_of, k), (B[k], buddy_of, k)])
        elif k < 8:
            got += [O[k], M[k]]
        elif k < 12:
            got += [O[k]]
        else:
            got += [F[k - 12]]
            waiting.append((F[k - 12], diagonal_of, k - 12))
        if 4 <= k < 6:
            waiting.append((X[k], diagonal_of, k - 2))
        if 6 <= k < 10:
            waiting.append((X[k], near_across_of, k - 6))
        if 10 <= k:
            waiting.append((X[k], far_across_of, k - 10))
        if 4 <= k < 12:
            j = k - 4
            V[j] = jnp.where(outer, O[k], M[j])
            waiting.append((V[j], near_of if j < 4 else far_of, j % 4))
        return got

    def send(k, *ties):
        tie = lambda value: after(value, *ties) if ties else value
        if k < 4:
            X[k] = across(tie(own[k]))
        elif k < 6:
            X[k] = across(tie(B[k - 2]))
        else:
            X[k] = across(tie(V[k - 6]))
        if k < 4:
            B[k] = buddies(tie(own[k]))
        elif k < 12:
            O[k] = outward(tie(M[k - 4]))
        else:
            F[k - 12] = buddies(tie(X[k - 12]))
        if k < 4:
            M[k] = middle(tie(own[k]))
        elif k < 8:
            M[k] = middle(tie(B[k - 4]))

    def settle(count):
        done = []
        for _ in range(min(count, len(waiting))):
            chunk, shard_of, c = waiting.pop(0)
            wholes[c % 2], token = decode(wholes[c % 2], [chunk], ratios, me, [(shard_of, c)])
            done.append(token)
        return done

    send(0)
    tables.append(buddies(maxima))
    send(1)
    for k in range(14):
        got = arrived(k)
        if k == 0:
            got.append(tables[1])
            tables.append(skip(after(jnp.concatenate(tables, axis=0), *got)))
        if k == 1:
            got.append(tables[2])
            tables.append(across(after(jnp.concatenate(tables, axis=0), *got)))
        if k == 2:
            got.append(tables[3])
            ratios, factors = ratios_of(tables)
        if k + 2 < 14:
            send(k + 2, *got, *tokens)
        if k == 2:
            *wholes, token = own_share(me, 8, w_gate, avg_gate, w_up, avg_up, norm_gain, factors, block // 2)
            tokens = [token]
        if k >= 3:
            tokens = settle(3 if k < 13 else len(waiting) - 2)
    chunks, shards_of, cs = zip(*waiting)
    t = cs[0] % 2
    wholes[t], _ = decode(wholes[t], chunks, ratios, me, list(zip(shards_of, cs)))
    return (*wholes, factors[0], factors[1])


def local_any(w_gate, avg_gate, w_up, avg_up, norm_gain):
    fresh_gained_gate = (keep_rate * avg_gate + (1.0 - keep_rate) * w_gate) * norm_gain[:, None]
    fresh_gained_up = (keep_rate * avg_up + (1.0 - keep_rate) * w_up) * norm_gain[:, None]
    factor_gate, factor_up = lax.pmax(
        (jnp.max(jnp.abs(fresh_gained_gate), axis=0), jnp.max(jnp.abs(fresh_gained_up), axis=0)),
        "rows",
    )
    serve_gate = lax.all_gather((fresh_gained_gate / factor_gate).astype(jnp.bfloat16), "rows", axis=0, tiled=True)
    serve_up = lax.all_gather((fresh_gained_up / factor_up).astype(jnp.bfloat16), "rows", axis=0, tiled=True)
    return serve_gate, serve_up, factor_gate, factor_up


def solution(mesh):
    plane = mesh.shape["rows"] == 8

    def local(*args):
        return (local_plane if plane else local_any)(*args)

    return jax.shard_map(
        local,
        mesh=mesh,
        in_specs=(P("rows", "width"),) * 4 + (P("rows"),),
        out_specs=(P(None, "width"), P(None, "width"), P("width"), P("width")),
        check_vma=False,
    )
```

```python
import functools

import jax
import jax.numpy as jnp
from jax import lax
from jax.experimental import pallas as pl
from jax.experimental.pallas import tpu as pltpu
from jax.sharding import PartitionSpec as P


keep_rate = 0.7

SPAN = 250.0
SCALE_OF_CHUNK = (0, 1, 2, 1)


KERNEL_VMEM = 14 * 2**20


def near_by(value):
    return pltpu.with_memory_space_constraint(value, pltpu.VMEM)


def stay_out(value):
    return pltpu.with_memory_space_constraint(value, pltpu.HBM)


def gained(w_ref, a_ref, gain):
    fresh = keep_rate * a_ref[...] + (1.0 - keep_rate) * w_ref[...]
    return fresh * gain


def tall_gain(gain_ref, width):
    rows = gain_ref.shape[0]
    lanes = jnp.broadcast_to(gain_ref[...].reshape(1, rows), (128, rows)).T
    return jnp.concatenate([lanes] * (width // 128), axis=1)


def scale_of(m):
    return m.astype(jnp.bfloat16).astype(jnp.float32)


def largest(x):
    return jnp.max(jnp.abs(x), axis=0, keepdims=True)


def coded(x, m):
    y = jnp.exp2(jnp.abs(x) * (SPAN / jnp.maximum(scale_of(m), 1e-30)) - SPAN / 2)
    return jnp.where(x < 0, -y, y).astype(jnp.bfloat16)


def encode_rest_body(gain_ref, wu0, au0, wg, ag, wu1, au1, first_ref, up0, gate, up1, m_ref):
    half_rows, width = wg.shape
    tall = tall_gain(gain_ref, width)
    top, bottom = tall[:half_rows], tall[half_rows:]
    upper, lower = gained(wu0, au0, top), gained(wu1, au1, bottom)
    m = jnp.maximum(largest(upper), largest(lower))
    up0[...] = coded(upper, m)
    up1[...] = coded(lower, m)
    m_ref[1] = m
    x = gained(wg, ag, bottom)
    m = largest(x)
    gate[...] = coded(x, m)
    m_ref[2] = m
    m_ref[0] = first_ref[0]


def encode_rest(w_gate, avg_gate, w_up, avg_up, gain, first_maxima, block):
    half_rows, columns = w_gate.shape[0] // 2, w_gate.shape[1]
    half = lambda h: [pl.BlockSpec((half_rows, block), lambda j: (h, j))] * 2
    stacked = lambda n: pl.BlockSpec((n, 1, block), lambda j: (0, 0, j))
    chunk = jax.ShapeDtypeStruct((half_rows, columns), jnp.bfloat16)
    return pl.pallas_call(
        encode_rest_body,
        grid=(columns // block,),
        in_specs=[pl.BlockSpec(gain.shape, lambda j: (0,)), *half(0), *half(1), *half(1), stacked(1)],
        out_specs=[pl.BlockSpec((half_rows, block), lambda j: (0, j))] * 3 + [stacked(3)],
        out_shape=[chunk, chunk, chunk, jax.ShapeDtypeStruct((3, 1, columns), jnp.float32)],
        compiler_params=pltpu.CompilerParams(vmem_limit_bytes=KERNEL_VMEM),
        name="encode_rest",
    )(gain, *map(stay_out, (w_up, avg_up, w_gate, avg_gate, w_up, avg_up)), near_by(first_maxima))


def encode_first_body(g_ref, w_ref, a_ref, y_ref, m_ref, gain_ref, ws, avgs, sems, *, half):
    half_rows, _ = y_ref.shape
    steps, _, width = ws.shape
    copies = []
    gain_copy = pltpu.make_async_copy(g_ref, gain_ref, sems.at[2, 0])
    gain_copy.start()
    for j in range(steps):
        source = (pl.ds(half * half_rows, half_rows), pl.ds(j * width, width))
        pair = [
            pltpu.make_async_copy(ref.at[source], held.at[j], sems.at[i, j])
            for i, (ref, held) in enumerate(((w_ref, ws), (a_ref, avgs)))
        ]
        for copy in pair:
            copy.start()
        copies.append(pair)
    gain_copy.wait()
    gain = tall_gain(gain_ref, width)[half * half_rows : (half + 1) * half_rows]
    for j, pair in enumerate(copies):
        for copy in pair:
            copy.wait()
        part = pl.ds(j * width, width)
        x = gained(ws.at[j], avgs.at[j], gain)
        m = largest(x)
        y_ref[:, part] = coded(x, m)
        m_ref[0, :, part] = m


def encode_first(w, avg, gain, half, width):
    half_rows, columns = w.shape[0] // 2, w.shape[1]
    here = pl.BlockSpec(memory_space=pltpu.VMEM)
    there = pl.BlockSpec(memory_space=pl.ANY)
    held = pltpu.VMEM((columns // width, half_rows, width), jnp.float32)
    return pl.pallas_call(
        functools.partial(encode_first_body, half=half),
        in_specs=[there, there, there],
        out_specs=[here, here],
        out_shape=[
            pltpu.VMEM((half_rows, columns), jnp.bfloat16),
            pltpu.VMEM((1, 1, columns), jnp.float32),
        ],
        scratch_shapes=[pltpu.VMEM(gain.shape, gain.dtype), held, held, pltpu.SemaphoreType.DMA((3, columns // width))],
        compiler_params=pltpu.CompilerParams(vmem_limit_bytes=KERNEL_VMEM),
        name="encode_first",
    )(stay_out(gain), stay_out(w), stay_out(avg))


def own_body(me_ref, wg_ref, ag_ref, wu_ref, au_ref, g_ref, f_ref, og_ref, ou_ref, token_ref):
    del me_ref
    gain = tall_gain(g_ref, wg_ref.shape[1])
    og_ref[...] = (gained(wg_ref, ag_ref, gain) / f_ref[0:1, :]).astype(jnp.bfloat16)
    ou_ref[...] = (gained(wu_ref, au_ref, gain) / f_ref[1:2, :]).astype(jnp.bfloat16)
    token_ref[...] = jnp.zeros_like(token_ref)


def own_share(me, shards, w_gate, avg_gate, w_up, avg_up, gain, factors, block):
    rows, columns = w_gate.shape
    tile = pl.BlockSpec((rows, block), lambda j, me: (0, j))
    landed = pl.BlockSpec((rows, block), lambda j, me: (me[0], j))
    out = jax.ShapeDtypeStruct((rows * shards, columns), jnp.bfloat16)
    return pl.pallas_call(
        own_body,
        grid_spec=pltpu.PrefetchScalarGridSpec(
            num_scalar_prefetch=1,
            grid=(columns // block,),
            in_specs=[tile] * 4
            + [
                pl.BlockSpec(gain.shape, lambda j, me: (0,)),
                pl.BlockSpec((2, block), lambda j, me: (0, j)),
            ],
            out_specs=[landed, landed, pl.BlockSpec((8, 128), lambda j, me: (0, 0))],
        ),
        out_shape=[out, out, jax.ShapeDtypeStruct((8, 128), jnp.float32)],
        compiler_params=pltpu.CompilerParams(vmem_limit_bytes=KERNEL_VMEM),
        name="own_share",
    )(me, *map(stay_out, (w_gate, avg_gate, w_up, avg_up)), gain, factors)


def half_table_body(m0_ref, m1_ref, m2_ref, scale_ref, most_ref):
    rows = [ref[i] for ref in (m0_ref, m1_ref, m2_ref) for i in range(ref.shape[0])]
    for i, row in enumerate(rows):
        scale_ref[i] = row.astype(jnp.bfloat16)
    most_ref[0] = functools.reduce(jnp.maximum, rows[0::3] + rows[2::3])
    most_ref[1] = functools.reduce(jnp.maximum, rows[1::3])


def half_table(maxima):
    columns = maxima[0].shape[-1]
    return pl.pallas_call(
        half_table_body,
        out_shape=[
            pltpu.VMEM((12, 1, columns), jnp.bfloat16),
            pltpu.VMEM((2, 1, columns), jnp.float32),
        ],
        compiler_params=pltpu.CompilerParams(vmem_limit_bytes=KERNEL_VMEM),
        name="half_table",
    )(*map(near_by, maxima))


def ratios_body(scale0_ref, scale1_ref, most0_ref, most1_ref, ratio_ref, factor_ref):
    for t in range(2):
        factor = jnp.maximum(most0_ref[t], most1_ref[t])
        factor_ref[t : t + 1, :] = factor
        for side, scale_ref in enumerate((scale0_ref, scale1_ref)):
            for place in range(4):
                for k in (0, 2) if t == 0 else (1,):
                    ratio_ref[3 * (2 * place + side) + k] = scale_ref[3 * place + k].astype(jnp.float32) / factor


def ratios_of(scales, most):
    columns = most[0].shape[-1]
    return pl.pallas_call(
        ratios_body,
        out_shape=[
            pltpu.VMEM((24, 1, columns), jnp.float32),
            jax.ShapeDtypeStruct((2, columns), jnp.float32),
        ],
        compiler_params=pltpu.CompilerParams(vmem_limit_bytes=KERNEL_VMEM),
        name="ratios",
    )(*map(near_by, scales), *map(near_by, most))


def decoded(y, ratio):
    y = y.astype(jnp.float32)
    x = jnp.log2(jnp.abs(y)) * (ratio * (1.0 / SPAN)) + ratio * 0.5
    return jnp.where(y < 0, -x, x).astype(jnp.bfloat16)


def decode_body(me_ref, r_ref, *refs, places, pieces):
    count = len(places)
    chunks, (out_ref, token_ref, buffer, sems) = refs[:count], refs[count + 1 :]
    rows = chunks[0].shape[0] // pieces
    me = me_ref[0]
    copies = []
    for i, (shard_of, c) in enumerate(places):
        shard = shard_of(me)
        ratio = r_ref[(shard ^ me) * 3 + SCALE_OF_CHUNK[c]]
        start = (2 * shard + c // 2) * chunks[0].shape[0]
        for p in range(pieces):
            part = pl.ds(p * rows, rows)
            buffer[i, part] = decoded(chunks[i][part], ratio)
            copies.append(
                pltpu.make_async_copy(buffer.at[i, part], out_ref.at[pl.ds(start + p * rows, rows)], sems.at[i, p])
            )
            copies[-1].start()
    token_ref[...] = jnp.zeros_like(token_ref)
    for copy in copies:
        copy.wait()


def decode(whole, chunks, ratios, me, places, pieces=4):
    here = pl.BlockSpec(memory_space=pltpu.VMEM)
    there = pl.BlockSpec(memory_space=pl.ANY)
    return pl.pallas_call(
        functools.partial(decode_body, places=places, pieces=pieces),
        in_specs=[pl.BlockSpec(memory_space=pltpu.SMEM), here] + [here] * len(chunks) + [there],
        out_specs=[there, here],
        out_shape=[
            jax.ShapeDtypeStruct(whole.shape, whole.dtype),
            pltpu.VMEM((8, 128), jnp.float32),
        ],
        scratch_shapes=[
            pltpu.VMEM((len(chunks), *chunks[0].shape), whole.dtype),
            pltpu.SemaphoreType.DMA((len(chunks), pieces)),
        ],
        input_output_aliases={2 + len(chunks): 0},
        compiler_params=pltpu.CompilerParams(vmem_limit_bytes=KERNEL_VMEM),
        name="decode",
    )(me, near_by(ratios), *map(near_by, chunks), whole)


def after(value, *tokens):
    return lax.optimization_barrier((value, *tokens))[0]


def across_of(me):
    return me ^ 1


def buddy_of(me):
    return me ^ 2


def diagonal_of(me):
    return me ^ 3


def near_of(me):
    return jnp.where(me < 4, 4, 2) + (me & 1)


def far_of(me):
    return jnp.where(me < 4, 6, 0) + (me & 1)


def near_across_of(me):
    return near_of(me) ^ 1


def far_across_of(me):
    return far_of(me) ^ 1


def local_plane(w_gate, avg_gate, w_up, avg_up, norm_gain):
    block = min(w_gate.shape[1], 1024)
    width = lax.axis_size("width")
    index = lax.axis_index("rows")
    outer = (index < 2) | (index >= 6)
    me = jnp.reshape(index, (1,)).astype(jnp.int32)

    def hop(value, pairs):
        both = [(2 * a + side, 2 * b + side) for a, b in pairs for side in (0, 1)]
        return lax.ppermute(value, "rows", both)

    across = lambda value: lax.ppermute(value, "rows", [(i, i ^ 1) for i in range(8)])
    buddies = lambda value: hop(value, [(0, 1), (1, 0), (2, 3), (3, 2)])
    outward = lambda value: hop(value, [(1, 0), (2, 3)])
    middle = lambda value: hop(value, [(1, 2), (2, 1)])
    skip = lambda value: hop(value, [(0, 2), (2, 0), (1, 3), (3, 1)])

    first, first_maxima = encode_first(w_gate, avg_gate, norm_gain, 0, block // 4)
    *rest, maxima = encode_rest(w_gate, avg_gate, w_up, avg_up, norm_gain, first_maxima, block // 2)
    own = [first, *rest]

    X, B, M, O, V, F = {}, {}, {}, {}, {}, {}
    tables = [maxima]
    factors = ratios = None
    wholes, tokens, waiting = [None, None], [], []

    def arrived(k):
        got = [X[k]]
        if k < 4:
            got += [B[k], M[k]]
            waiting.extend([(X[k], across_of, k), (B[k], buddy_of, k)])
        elif k < 8:
            got += [O[k], M[k]]
        elif k < 12:
            got += [O[k]]
        else:
            got += [F[k - 12]]
            waiting.append((F[k - 12], diagonal_of, k - 12))
        if 4 <= k < 6:
            waiting.append((X[k], diagonal_of, k - 2))
        if 6 <= k < 10:
            waiting.append((X[k], near_across_of, k - 6))
        if 10 <= k:
            waiting.append((X[k], far_across_of, k - 10))
        if 4 <= k < 12:
            j = k - 4
            V[j] = jnp.where(outer, O[k], M[j])
            waiting.append((V[j], near_of if j < 4 else far_of, j % 4))
        return got

    def send_first():
        odd = lax.axis_index("width") % 2 == 1
        cores = [(row, column) for row in range(8) for column in range(width)]
        flat = lambda row, column: row * width + column
        swap = lambda turn: lax.ppermute(
            first,
            ("rows", "width"),
            [(flat(r, c), flat(r ^ (1 if (c + turn) % 2 == 0 else 2), c)) for r, c in cores],
        )
        one = swap(0)
        two = swap(1)
        M[0] = middle(first)
        X[0] = jnp.where(odd, two, one)
        B[0] = jnp.where(odd, one, two)

    def send(k, *ties):
        tie = lambda value: after(value, *ties) if ties else value
        if k < 4:
            X[k] = across(tie(own[k]))
        elif k < 6:
            X[k] = across(tie(B[k - 2]))
        else:
            X[k] = across(tie(V[k - 6]))
        if k < 4:
            B[k] = buddies(tie(own[k]))
        elif k < 12:
            O[k] = outward(tie(M[k - 4]))
        else:
            F[k - 12] = buddies(tie(X[k - 12]))
        if k < 4:
            M[k] = middle(tie(own[k]))
        elif k < 8:
            M[k] = middle(tie(B[k - 4]))

    def settle(count):
        done = []
        for _ in range(min(count, len(waiting))):
            chunk, shard_of, c = waiting.pop(0)
            wholes[c % 2], token = decode(wholes[c % 2], [chunk], ratios, me, [(shard_of, c)])
            done.append(token)
        return done

    send_first()
    tables.append(buddies(maxima))
    send(1)
    for k in range(14):
        got = arrived(k)
        if k == 0:
            got.append(tables[1])
            tables.append(skip(after(jnp.concatenate(tables, axis=0), *got)))
        if k == 1:
            got.append(tables[2])
            scales, most = half_table(tables)
            far_scales = across(after(scales, *got))
            far_most = across(after(most, *got))
        if k == 2:
            got += [far_scales, far_most]
            ratios, factors = ratios_of((scales, far_scales), (most, far_most))
        if k + 2 < 14:
            send(k + 2, *got, *tokens)
        if k == 2:
            *wholes, token = own_share(me, 8, w_gate, avg_gate, w_up, avg_up, norm_gain, factors, block // 2)
            tokens = [token]
        if k >= 3:
            tokens = settle(3 if k < 13 else len(waiting) - 2)
    chunks, shards_of, cs = zip(*waiting)
    t = cs[0] % 2
    wholes[t], _ = decode(wholes[t], chunks, ratios, me, list(zip(shards_of, cs)))
    return (*wholes, factors[0], factors[1])


def local_any(w_gate, avg_gate, w_up, avg_up, norm_gain):
    fresh_gained_gate = (keep_rate * avg_gate + (1.0 - keep_rate) * w_gate) * norm_gain[:, None]
    fresh_gained_up = (keep_rate * avg_up + (1.0 - keep_rate) * w_up) * norm_gain[:, None]
    factor_gate, factor_up = lax.pmax(
        (jnp.max(jnp.abs(fresh_gained_gate), axis=0), jnp.max(jnp.abs(fresh_gained_up), axis=0)),
        "rows",
    )
    serve_gate = lax.all_gather((fresh_gained_gate / factor_gate).astype(jnp.bfloat16), "rows", axis=0, tiled=True)
    serve_up = lax.all_gather((fresh_gained_up / factor_up).astype(jnp.bfloat16), "rows", axis=0, tiled=True)
    return serve_gate, serve_up, factor_gate, factor_up


def solution(mesh):
    plane = mesh.shape["rows"] == 8

    def local(*args):
        return (local_plane if plane else local_any)(*args)

    return jax.shard_map(
        local,
        mesh=mesh,
        in_specs=(P("rows", "width"),) * 4 + (P("rows"),),
        out_specs=(P(None, "width"), P(None, "width"), P("width"), P("width")),
        check_vma=False,
    )
```

```python
import functools

import jax
import jax.numpy as jnp
from jax import lax
from jax.experimental import pallas as pl
from jax.experimental.pallas import tpu as pltpu
from jax.sharding import PartitionSpec as P


keep_rate = 0.7

SPAN = 250.0
SCALE_OF_CHUNK = (0, 1, 2, 1)


KERNEL_VMEM = 14 * 2**20


def near_by(value):
    return pltpu.with_memory_space_constraint(value, pltpu.VMEM)


def stay_out(value):
    return pltpu.with_memory_space_constraint(value, pltpu.HBM)


def gained(w_ref, a_ref, gain):
    fresh = keep_rate * a_ref[...] + (1.0 - keep_rate) * w_ref[...]
    return fresh * gain


def tall_gain(gain_ref, width):
    rows = gain_ref.shape[0]
    lanes = jnp.broadcast_to(gain_ref[...].reshape(1, rows), (128, rows)).T
    return jnp.concatenate([lanes] * (width // 128), axis=1)


def scale_of(m):
    return m.astype(jnp.bfloat16).astype(jnp.float32)


def largest(x):
    return jnp.max(jnp.abs(x), axis=0, keepdims=True)


def coded(x, m):
    y = jnp.exp2(jnp.abs(x) * (SPAN / jnp.maximum(scale_of(m), 1e-30)) - SPAN / 2)
    return jnp.where(x < 0, -y, y).astype(jnp.bfloat16)


def encode_rest_body(gain_ref, wu0, au0, wg, ag, wu1, au1, first_ref, up0, gate, up1, m_ref):
    half_rows, width = wg.shape
    tall = tall_gain(gain_ref, width)
    top, bottom = tall[:half_rows], tall[half_rows:]
    upper, lower = gained(wu0, au0, top), gained(wu1, au1, bottom)
    m = jnp.maximum(largest(upper), largest(lower))
    up0[...] = coded(upper, m)
    up1[...] = coded(lower, m)
    m_ref[1] = m
    x = gained(wg, ag, bottom)
    m = largest(x)
    gate[...] = coded(x, m)
    m_ref[2] = m
    m_ref[0] = first_ref[0]


def encode_rest(w_gate, avg_gate, w_up, avg_up, gain, first_maxima, block):
    half_rows, columns = w_gate.shape[0] // 2, w_gate.shape[1]
    half = lambda h: [pl.BlockSpec((half_rows, block), lambda j: (h, j))] * 2
    stacked = lambda n: pl.BlockSpec((n, 1, block), lambda j: (0, 0, j))
    chunk = jax.ShapeDtypeStruct((half_rows, columns), jnp.bfloat16)
    return pl.pallas_call(
        encode_rest_body,
        grid=(columns // block,),
        in_specs=[pl.BlockSpec(gain.shape, lambda j: (0,)), *half(0), *half(1), *half(1), stacked(1)],
        out_specs=[pl.BlockSpec((half_rows, block), lambda j: (0, j))] * 3 + [stacked(3)],
        out_shape=[chunk, chunk, chunk, jax.ShapeDtypeStruct((3, 1, columns), jnp.float32)],
        compiler_params=pltpu.CompilerParams(vmem_limit_bytes=KERNEL_VMEM),
        name="encode_rest",
    )(gain, *map(stay_out, (w_up, avg_up, w_gate, avg_gate, w_up, avg_up)), near_by(first_maxima))


def encode_first_body(g_ref, w_ref, a_ref, y_ref, m_ref, gain_ref, ws, avgs, sems, *, half):
    half_rows, _ = y_ref.shape
    steps, _, width = ws.shape
    copies = []
    gain_copy = pltpu.make_async_copy(g_ref, gain_ref, sems.at[2, 0])
    gain_copy.start()
    for j in range(steps):
        source = (pl.ds(half * half_rows, half_rows), pl.ds(j * width, width))
        pair = [
            pltpu.make_async_copy(ref.at[source], held.at[j], sems.at[i, j])
            for i, (ref, held) in enumerate(((w_ref, ws), (a_ref, avgs)))
        ]
        for copy in pair:
            copy.start()
        copies.append(pair)
    gain_copy.wait()
    gain = tall_gain(gain_ref, width)[half * half_rows : (half + 1) * half_rows]
    for j, pair in enumerate(copies):
        for copy in pair:
            copy.wait()
        part = pl.ds(j * width, width)
        x = gained(ws.at[j], avgs.at[j], gain)
        m = largest(x)
        y_ref[:, part] = coded(x, m)
        m_ref[0, :, part] = m


def encode_first(w, avg, gain, half, width):
    half_rows, columns = w.shape[0] // 2, w.shape[1]
    here = pl.BlockSpec(memory_space=pltpu.VMEM)
    there = pl.BlockSpec(memory_space=pl.ANY)
    held = pltpu.VMEM((columns // width, half_rows, width), jnp.float32)
    return pl.pallas_call(
        functools.partial(encode_first_body, half=half),
        in_specs=[there, there, there],
        out_specs=[here, here],
        out_shape=[
            pltpu.VMEM((half_rows, columns), jnp.bfloat16),
            pltpu.VMEM((1, 1, columns), jnp.float32),
        ],
        scratch_shapes=[pltpu.VMEM(gain.shape, gain.dtype), held, held, pltpu.SemaphoreType.DMA((3, columns // width))],
        compiler_params=pltpu.CompilerParams(vmem_limit_bytes=KERNEL_VMEM),
        name="encode_first",
    )(stay_out(gain), stay_out(w), stay_out(avg))


def half_table_body(m0_ref, m1_ref, m2_ref, scale_ref, most_ref):
    rows = [ref[i] for ref in (m0_ref, m1_ref, m2_ref) for i in range(ref.shape[0])]
    rest = [jnp.zeros_like(rows[0])] * (scale_ref.shape[0] - len(rows))
    scale_ref[...] = jnp.concatenate(rows + rest, axis=0).astype(jnp.bfloat16)
    most_ref[0] = functools.reduce(jnp.maximum, rows[0::3] + rows[2::3])
    most_ref[1] = functools.reduce(jnp.maximum, rows[1::3])


def half_table(maxima):
    columns = maxima[0].shape[-1]
    return pl.pallas_call(
        half_table_body,
        out_shape=[
            pltpu.VMEM((16, columns), jnp.bfloat16),
            pltpu.VMEM((2, 1, columns), jnp.float32),
        ],
        compiler_params=pltpu.CompilerParams(vmem_limit_bytes=KERNEL_VMEM),
        name="half_table",
    )(*map(near_by, maxima))


def ratios_body(scale0_ref, scale1_ref, most0_ref, most1_ref, ratio_ref, factor_ref):
    for t in range(2):
        factor = jnp.maximum(most0_ref[t], most1_ref[t])
        factor_ref[t : t + 1, :] = factor
        for side, scale_ref in enumerate((scale0_ref, scale1_ref)):
            scales = scale_ref[...].astype(jnp.float32)
            for place in range(4):
                for k in (3 * place, 3 * place + 2) if t == 0 else (3 * place + 1,):
                    ratio_ref[3 * place + 3 * side + k] = scales[k : k + 1] / factor


def ratios_of(scales, most):
    columns = most[0].shape[-1]
    return pl.pallas_call(
        ratios_body,
        out_shape=[
            pltpu.VMEM((24, 1, columns), jnp.float32),
            jax.ShapeDtypeStruct((2, columns), jnp.float32),
        ],
        compiler_params=pltpu.CompilerParams(vmem_limit_bytes=KERNEL_VMEM),
        name="ratios",
    )(*map(near_by, scales), *map(near_by, most))


def decoded(y, ratio):
    y = y.astype(jnp.float32)
    x = jnp.log2(jnp.abs(y)) * (ratio * (1.0 / SPAN)) + ratio * 0.5
    return jnp.where(y < 0, -x, x).astype(jnp.bfloat16)


def decode_body(me_ref, r_ref, *refs, places, pieces):
    count = len(places)
    chunks, (out_ref, token_ref, buffer, sems) = refs[:count], refs[-4:]
    rows = chunks[0].shape[0] // pieces
    me = me_ref[0]
    copies = []
    for i, (shard_of, c) in enumerate(places):
        shard = shard_of(me)
        ratio = r_ref[(shard ^ me) * 3 + SCALE_OF_CHUNK[c]]
        start = (2 * shard + c // 2) * chunks[0].shape[0]
        for p in range(pieces):
            part = pl.ds(p * rows, rows)
            buffer[i, part] = decoded(chunks[i][part], ratio)
            copies.append(
                pltpu.make_async_copy(buffer.at[i, part], out_ref.at[pl.ds(start + p * rows, rows)], sems.at[i, p])
            )
            copies[-1].start()
    token_ref[...] = jnp.zeros_like(token_ref)
    for copy in copies:
        copy.wait()


def decode(whole, chunks, ratios, me, places, pieces=4):
    here = pl.BlockSpec(memory_space=pltpu.VMEM)
    there = pl.BlockSpec(memory_space=pl.ANY)
    begun = not isinstance(whole, jax.ShapeDtypeStruct)
    return pl.pallas_call(
        functools.partial(decode_body, places=places, pieces=pieces),
        in_specs=[pl.BlockSpec(memory_space=pltpu.SMEM), here] + [here] * len(chunks) + [there] * begun,
        out_specs=[there, here],
        out_shape=[
            jax.ShapeDtypeStruct(whole.shape, whole.dtype),
            pltpu.VMEM((8, 128), jnp.float32),
        ],
        scratch_shapes=[
            pltpu.VMEM((len(chunks), *chunks[0].shape), whole.dtype),
            pltpu.SemaphoreType.DMA((len(chunks), pieces)),
        ],
        input_output_aliases={2 + len(chunks): 0} if begun else {},
        compiler_params=pltpu.CompilerParams(vmem_limit_bytes=KERNEL_VMEM),
        name="decode",
    )(me, near_by(ratios), *map(near_by, chunks), *[whole] * begun)


def after(value, *tokens):
    return lax.optimization_barrier((value, *tokens))[0]


def own_of(me):
    return me


def across_of(me):
    return me ^ 1


def buddy_of(me):
    return me ^ 2


def diagonal_of(me):
    return me ^ 3


def near_of(me):
    return jnp.where(me < 4, 4, 2) + (me & 1)


def far_of(me):
    return jnp.where(me < 4, 6, 0) + (me & 1)


def near_across_of(me):
    return near_of(me) ^ 1


def far_across_of(me):
    return far_of(me) ^ 1


def local_plane(w_gate, avg_gate, w_up, avg_up, norm_gain):
    rows, columns = w_gate.shape
    block = min(columns, 1024)
    width = lax.axis_size("width")
    index = lax.axis_index("rows")
    outer = (index < 2) | (index >= 6)
    me = jnp.reshape(index, (1,)).astype(jnp.int32)

    def hop(value, pairs):
        both = [(2 * a + side, 2 * b + side) for a, b in pairs for side in (0, 1)]
        return lax.ppermute(value, "rows", both)

    across = lambda value: lax.ppermute(value, "rows", [(i, i ^ 1) for i in range(8)])
    buddies = lambda value: hop(value, [(0, 1), (1, 0), (2, 3), (3, 2)])
    outward = lambda value: hop(value, [(1, 0), (2, 3)])
    middle = lambda value: hop(value, [(1, 2), (2, 1)])
    skip = lambda value: hop(value, [(0, 2), (2, 0), (1, 3), (3, 1)])

    first, first_maxima = encode_first(w_gate, avg_gate, norm_gain, 0, block // 4)
    *rest, maxima = encode_rest(w_gate, avg_gate, w_up, avg_up, norm_gain, first_maxima, block // 2)
    own = [first, *rest]

    X, B, M, O, V, F = {}, {}, {}, {}, {}, {}
    tables = [maxima]
    factors = ratios = None
    wholes, tokens, waiting = [None, None], [], []

    def arrived(k):
        got = [X[k]]
        if k < 4:
            got += [B[k], M[k]]
            waiting.extend([(X[k], across_of, k), (B[k], buddy_of, k)])
        elif k < 8:
            got += [O[k], M[k]]
        elif k < 12:
            got += [O[k]]
        else:
            got += [F[k - 12]]
            waiting.append((F[k - 12], diagonal_of, k - 12))
        if 4 <= k < 6:
            waiting.append((X[k], diagonal_of, k - 2))
        if 6 <= k < 10:
            waiting.append((X[k], near_across_of, k - 6))
        if 10 <= k:
            waiting.append((X[k], far_across_of, k - 10))
        if 4 <= k < 12:
            j = k - 4
            V[j] = jnp.where(outer, O[k], M[j])
            waiting.append((V[j], near_of if j < 4 else far_of, j % 4))
        return got

    def send_first():
        odd = lax.axis_index("width") % 2 == 1
        cores = [(row, column) for row in range(8) for column in range(width)]
        flat = lambda row, column: row * width + column
        swap = lambda turn: lax.ppermute(
            first,
            ("rows", "width"),
            [(flat(r, c), flat(r ^ (1 if (c + turn) % 2 == 0 else 2), c)) for r, c in cores],
        )
        one = swap(0)
        two = swap(1)
        M[0] = middle(first)
        X[0] = jnp.where(odd, two, one)
        B[0] = jnp.where(odd, one, two)

    def send(k, *ties):
        tie = lambda value: after(value, *ties) if ties else value
        if k < 4:
            X[k] = across(tie(own[k]))
        elif k < 6:
            X[k] = across(tie(B[k - 2]))
        else:
            X[k] = across(tie(V[k - 6]))
        if k < 4:
            B[k] = buddies(tie(own[k]))
        elif k < 12:
            O[k] = outward(tie(M[k - 4]))
        else:
            F[k - 12] = buddies(tie(X[k - 12]))
        if k < 4:
            M[k] = middle(tie(own[k]))
        elif k < 8:
            M[k] = middle(tie(B[k - 4]))

    def settle(count):
        done = []
        for _ in range(min(count, len(waiting))):
            chunk, shard_of, c = waiting.pop(0)
            wholes[c % 2], token = decode(wholes[c % 2], [chunk], ratios, me, [(shard_of, c)])
            done.append(token)
        return done

    send_first()
    tables.append(buddies(maxima))
    send(1)
    for k in range(14):
        got = arrived(k)
        if k == 0:
            got.append(tables[1])
            tables.append(skip(after(jnp.concatenate(tables, axis=0), *got)))
        if k == 1:
            got.append(tables[2])
            scales, most = half_table(tables)
            far_scales = across(after(scales, *got))
            far_most = across(after(most, *got))
        if k == 2:
            got += [far_scales, far_most]
            ratios, factors = ratios_of((scales, far_scales), (most, far_most))
        if k + 2 < 14:
            send(k + 2, *got, *tokens)
        if k == 2:
            out = jax.ShapeDtypeStruct((8 * rows, columns), jnp.bfloat16)
            wholes, tokens = zip(*[decode(out, own[t::2], ratios, me, [(own_of, t), (own_of, t + 2)]) for t in (0, 1)])
            wholes = list(wholes)
        if k >= 3:
            tokens = settle(3 if k < 13 else len(waiting) - 2)
    chunks, shards_of, cs = zip(*waiting)
    t = cs[0] % 2
    wholes[t], _ = decode(wholes[t], chunks, ratios, me, list(zip(shards_of, cs)))
    return (*wholes, factors[0], factors[1])


def local_any(w_gate, avg_gate, w_up, avg_up, norm_gain):
    fresh_gained_gate = (keep_rate * avg_gate + (1.0 - keep_rate) * w_gate) * norm_gain[:, None]
    fresh_gained_up = (keep_rate * avg_up + (1.0 - keep_rate) * w_up) * norm_gain[:, None]
    factor_gate, factor_up = lax.pmax(
        (jnp.max(jnp.abs(fresh_gained_gate), axis=0), jnp.max(jnp.abs(fresh_gained_up), axis=0)),
        "rows",
    )
    serve_gate = lax.all_gather((fresh_gained_gate / factor_gate).astype(jnp.bfloat16), "rows", axis=0, tiled=True)
    serve_up = lax.all_gather((fresh_gained_up / factor_up).astype(jnp.bfloat16), "rows", axis=0, tiled=True)
    return serve_gate, serve_up, factor_gate, factor_up


def solution(mesh):
    plane = mesh.shape["rows"] == 8

    def local(*args):
        return (local_plane if plane else local_any)(*args)

    return jax.shard_map(
        local,
        mesh=mesh,
        in_specs=(P("rows", "width"),) * 4 + (P("rows"),),
        out_specs=(P(None, "width"), P(None, "width"), P("width"), P("width")),
        check_vma=False,
    )
```

```python
import functools

import jax
import jax.numpy as jnp
from jax import lax
from jax.experimental import pallas as pl
from jax.experimental.pallas import tpu as pltpu
from jax.sharding import PartitionSpec as P


keep_rate = 0.7

SPAN = 250.0
SCALE_OF_CHUNK = (0, 1, 2, 1)


KERNEL_VMEM = 14 * 2**20


def near_by(value):
    return pltpu.with_memory_space_constraint(value, pltpu.VMEM)


def stay_out(value):
    return pltpu.with_memory_space_constraint(value, pltpu.HBM)


def gained(w_ref, a_ref, gain):
    fresh = keep_rate * a_ref[...] + (1.0 - keep_rate) * w_ref[...]
    return fresh * gain


def tall_gain(gain_ref, width):
    rows = gain_ref.shape[0]
    lanes = jnp.broadcast_to(gain_ref[...].reshape(1, rows), (128, rows)).T
    return jnp.concatenate([lanes] * (width // 128), axis=1)


def scale_of(m):
    return m.astype(jnp.bfloat16).astype(jnp.float32)


def largest(x):
    return jnp.max(jnp.abs(x), axis=0, keepdims=True)


def coded(x, m):
    y = jnp.exp2(jnp.abs(x) * (SPAN / jnp.maximum(scale_of(m), 1e-30)) - SPAN / 2)
    return jnp.where(x < 0, -y, y).astype(jnp.bfloat16)


def encode_rest_body(gain_ref, wu0, au0, wg, ag, wu1, au1, first_ref, up0, gate, up1, m_ref):
    half_rows, width = wg.shape
    tall = tall_gain(gain_ref, width)
    top, bottom = tall[:half_rows], tall[half_rows:]
    upper, lower = gained(wu0, au0, top), gained(wu1, au1, bottom)
    m = jnp.maximum(largest(upper), largest(lower))
    up0[...] = coded(upper, m)
    up1[...] = coded(lower, m)
    m_ref[1] = m
    x = gained(wg, ag, bottom)
    m = largest(x)
    gate[...] = coded(x, m)
    m_ref[2] = m
    m_ref[0] = first_ref[0]


def encode_rest(w_gate, avg_gate, w_up, avg_up, gain, first_maxima, block):
    half_rows, columns = w_gate.shape[0] // 2, w_gate.shape[1]
    half = lambda h: [pl.BlockSpec((half_rows, block), lambda j: (h, j))] * 2
    stacked = lambda n: pl.BlockSpec((n, 1, block), lambda j: (0, 0, j))
    chunk = jax.ShapeDtypeStruct((half_rows, columns), jnp.bfloat16)
    return pl.pallas_call(
        encode_rest_body,
        grid=(columns // block,),
        in_specs=[pl.BlockSpec(gain.shape, lambda j: (0,)), *half(0), *half(1), *half(1), stacked(1)],
        out_specs=[pl.BlockSpec((half_rows, block), lambda j: (0, j))] * 3 + [stacked(3)],
        out_shape=[chunk, chunk, chunk, jax.ShapeDtypeStruct((3, 1, columns), jnp.float32)],
        compiler_params=pltpu.CompilerParams(vmem_limit_bytes=KERNEL_VMEM),
        name="encode_rest",
    )(gain, *map(stay_out, (w_up, avg_up, w_gate, avg_gate, w_up, avg_up)), near_by(first_maxima))


def encode_first_body(g_ref, w_ref, a_ref, y_ref, m_ref, gain_ref, ws, avgs, sems, *, half):
    half_rows, _ = y_ref.shape
    steps, _, width = ws.shape
    copies = []
    gain_copy = pltpu.make_async_copy(g_ref, gain_ref, sems.at[2, 0])
    gain_copy.start()
    for j in range(steps):
        source = (pl.ds(half * half_rows, half_rows), pl.ds(j * width, width))
        pair = [
            pltpu.make_async_copy(ref.at[source], held.at[j], sems.at[i, j])
            for i, (ref, held) in enumerate(((w_ref, ws), (a_ref, avgs)))
        ]
        for copy in pair:
            copy.start()
        copies.append(pair)
    gain_copy.wait()
    gain = tall_gain(gain_ref, width)[half * half_rows : (half + 1) * half_rows]
    for j, pair in enumerate(copies):
        for copy in pair:
            copy.wait()
        part = pl.ds(j * width, width)
        x = gained(ws.at[j], avgs.at[j], gain)
        m = largest(x)
        y_ref[:, part] = coded(x, m)
        m_ref[0, :, part] = m


def encode_first(w, avg, gain, half, width):
    half_rows, columns = w.shape[0] // 2, w.shape[1]
    here = pl.BlockSpec(memory_space=pltpu.VMEM)
    there = pl.BlockSpec(memory_space=pl.ANY)
    held = pltpu.VMEM((columns // width, half_rows, width), jnp.float32)
    return pl.pallas_call(
        functools.partial(encode_first_body, half=half),
        in_specs=[there, there, there],
        out_specs=[here, here],
        out_shape=[
            pltpu.VMEM((half_rows, columns), jnp.bfloat16),
            pltpu.VMEM((1, 1, columns), jnp.float32),
        ],
        scratch_shapes=[pltpu.VMEM(gain.shape, gain.dtype), held, held, pltpu.SemaphoreType.DMA((3, columns // width))],
        compiler_params=pltpu.CompilerParams(vmem_limit_bytes=KERNEL_VMEM),
        name="encode_first",
    )(stay_out(gain), stay_out(w), stay_out(avg))


def half_table_body(m0_ref, m1_ref, m2_ref, scale_ref, most_ref):
    rows = [ref[i] for ref in (m0_ref, m1_ref, m2_ref) for i in range(ref.shape[0])]
    rest = [jnp.zeros_like(rows[0])] * (scale_ref.shape[0] - len(rows))
    scale_ref[...] = jnp.concatenate(rows + rest, axis=0).astype(jnp.bfloat16)
    most_ref[0] = functools.reduce(jnp.maximum, rows[0::3] + rows[2::3])
    most_ref[1] = functools.reduce(jnp.maximum, rows[1::3])


def half_table(maxima):
    columns = maxima[0].shape[-1]
    return pl.pallas_call(
        half_table_body,
        out_shape=[
            pltpu.VMEM((16, columns), jnp.bfloat16),
            pltpu.VMEM((2, 1, columns), jnp.float32),
        ],
        compiler_params=pltpu.CompilerParams(vmem_limit_bytes=KERNEL_VMEM),
        name="half_table",
    )(*map(near_by, maxima))


def ratios_body(scale0_ref, scale1_ref, most0_ref, most1_ref, ratio_ref, factor_ref):
    for t in range(2):
        factor = jnp.maximum(most0_ref[t], most1_ref[t])
        factor_ref[t : t + 1, :] = factor
        for side, scale_ref in enumerate((scale0_ref, scale1_ref)):
            scales = scale_ref[...].astype(jnp.float32)
            for place in range(4):
                for k in (3 * place, 3 * place + 2) if t == 0 else (3 * place + 1,):
                    ratio_ref[3 * place + 3 * side + k] = scales[k : k + 1] / factor


def ratios_of(scales, most):
    columns = most[0].shape[-1]
    return pl.pallas_call(
        ratios_body,
        out_shape=[
            pltpu.VMEM((24, 1, columns), jnp.float32),
            jax.ShapeDtypeStruct((2, columns), jnp.float32),
        ],
        compiler_params=pltpu.CompilerParams(vmem_limit_bytes=KERNEL_VMEM),
        name="ratios",
    )(*map(near_by, scales), *map(near_by, most))


def decoded(y, ratio):
    y = y.astype(jnp.float32)
    x = jnp.log2(jnp.abs(y)) * (ratio * (1.0 / SPAN)) + ratio * 0.5
    return jnp.where(y < 0, -x, x).astype(jnp.bfloat16)


def decode_body(me_ref, r_ref, *refs, places, pieces, half_rows):
    count = len(places)
    chunks, (out_ref, token_ref, buffer, sems) = refs[:count], refs[-4:]
    rows = chunks[0].shape[0] // pieces
    me = me_ref[0]
    copies = []
    for i, (shard_of, c, offset) in enumerate(places):
        shard = shard_of(me)
        ratio = r_ref[(shard ^ me) * 3 + SCALE_OF_CHUNK[c]]
        start = (2 * shard + c // 2) * half_rows + offset
        for p in range(pieces):
            part = pl.ds(p * rows, rows)
            buffer[i, part] = decoded(chunks[i][part], ratio)
            copies.append(
                pltpu.make_async_copy(buffer.at[i, part], out_ref.at[pl.ds(start + p * rows, rows)], sems.at[i, p])
            )
            copies[-1].start()
    token_ref[...] = jnp.zeros_like(token_ref)
    for copy in copies:
        copy.wait()


def decode(whole, chunks, ratios, me, places):
    here = pl.BlockSpec(memory_space=pltpu.VMEM)
    there = pl.BlockSpec(memory_space=pl.ANY)
    begun = not isinstance(whole, jax.ShapeDtypeStruct)
    half_rows, height = whole.shape[0] // 16, chunks[0].shape[0]
    pieces = next(n for n in (4, 3, 1) if height % (16 * n) == 0)
    return pl.pallas_call(
        functools.partial(decode_body, places=places, pieces=pieces, half_rows=half_rows),
        in_specs=[pl.BlockSpec(memory_space=pltpu.SMEM), here] + [here] * len(chunks) + [there] * begun,
        out_specs=[there, here],
        out_shape=[
            jax.ShapeDtypeStruct(whole.shape, whole.dtype),
            pltpu.VMEM((8, 128), jnp.float32),
        ],
        scratch_shapes=[
            pltpu.VMEM((len(chunks), *chunks[0].shape), whole.dtype),
            pltpu.SemaphoreType.DMA((len(chunks), pieces)),
        ],
        input_output_aliases={2 + len(chunks): 0} if begun else {},
        compiler_params=pltpu.CompilerParams(vmem_limit_bytes=KERNEL_VMEM),
        name="decode",
    )(me, near_by(ratios), *map(near_by, chunks), *[whole] * begun)


def after(value, *tokens):
    return lax.optimization_barrier((value, *tokens))[0]


def own_of(me):
    return me


def across_of(me):
    return me ^ 1


def buddy_of(me):
    return me ^ 2


def diagonal_of(me):
    return me ^ 3


def near_of(me):
    return jnp.where(me < 4, 4, 2) + (me & 1)


def far_of(me):
    return jnp.where(me < 4, 6, 0) + (me & 1)


def near_across_of(me):
    return near_of(me) ^ 1


def far_across_of(me):
    return far_of(me) ^ 1


def local_plane(w_gate, avg_gate, w_up, avg_up, norm_gain):
    rows, columns = w_gate.shape
    block = min(columns, 1024)
    cut = rows // 2 - rows // 128 * 16
    width = lax.axis_size("width")
    index = lax.axis_index("rows")
    outer = (index < 2) | (index >= 6)
    me = jnp.reshape(index, (1,)).astype(jnp.int32)

    def hop(value, pairs):
        both = [(2 * a + side, 2 * b + side) for a, b in pairs for side in (0, 1)]
        return lax.ppermute(value, "rows", both)

    across = lambda value: lax.ppermute(value, "rows", [(i, i ^ 1) for i in range(8)])
    buddies = lambda value: hop(value, [(0, 1), (1, 0), (2, 3), (3, 2)])
    outward = lambda value: hop(value, [(1, 0), (2, 3)])
    middle = lambda value: hop(value, [(1, 2), (2, 1)])
    skip = lambda value: hop(value, [(0, 2), (2, 0), (1, 3), (3, 1)])

    first, first_maxima = encode_first(w_gate, avg_gate, norm_gain, 0, block // 4)
    *rest, maxima = encode_rest(w_gate, avg_gate, w_up, avg_up, norm_gain, first_maxima, block // 2)
    own = [first, *rest]

    X, B, M, O, V, F = {}, {}, {}, {}, {}, {}
    tables = [maxima]
    factors = ratios = None
    wholes, tokens, waiting = [None, None], [], []

    def wait_for(chunk, shard_of, c, offset=0):
        waiting.append((chunk, (shard_of, c, offset)))

    def arrived(k):
        got = [X[k]]
        if k < 4:
            got += [B[k], M[k]]
            wait_for(X[k], across_of, k)
            wait_for(B[k], buddy_of, k)
        elif k < 8:
            got += [O[k], M[k]]
        elif k < 12:
            got += [O[k]]
        else:
            got += [F[0]]
            wait_for(F[0], diagonal_of, 0)
        if 4 <= k < 6:
            wait_for(X[k], diagonal_of, k - 2)
        if 6 <= k < 10:
            wait_for(X[k], near_across_of, k - 6)
        if 10 <= k:
            wait_for(X[k], far_across_of, k - 10)
        if 4 <= k < 12:
            j = k - 4
            V[j] = jnp.where(outer, O[k], M[j])
            wait_for(V[j], near_of if j < 4 else far_of, j % 4)
        return got

    def send_last(*ties):
        parts = [slice(0, cut), slice(cut, rows // 2)]
        for name, part in zip("ab", parts):
            X[name] = across(after(jnp.where(outer, O[11][part], M[7][part]), *ties))
            F[name] = buddies(after(X[1][part], *ties))

    def send_first():
        odd = lax.axis_index("width") % 2 == 1
        cores = [(row, column) for row in range(8) for column in range(width)]
        flat = lambda row, column: row * width + column
        swap = lambda turn: lax.ppermute(
            first,
            ("rows", "width"),
            [(flat(r, c), flat(r ^ (1 if (c + turn) % 2 == 0 else 2), c)) for r, c in cores],
        )
        one = swap(0)
        two = swap(1)
        M[0] = middle(first)
        X[0] = jnp.where(odd, two, one)
        B[0] = jnp.where(odd, one, two)

    def send(k, *ties):
        tie = lambda value: after(value, *ties) if ties else value
        if k < 4:
            X[k] = across(tie(own[k]))
        elif k < 6:
            X[k] = across(tie(B[k - 2]))
        else:
            X[k] = across(tie(V[k - 6]))
        if k < 4:
            B[k] = buddies(tie(own[k]))
        elif k < 12:
            O[k] = outward(tie(M[k - 4]))
        else:
            F[k - 12] = buddies(tie(X[k - 12]))
        if k < 4:
            M[k] = middle(tie(own[k]))
        elif k < 8:
            M[k] = middle(tie(B[k - 4]))

    def settle(count):
        done = []
        for _ in range(min(count, len(waiting))):
            chunk, place = waiting.pop(0)
            t = place[1] % 2
            wholes[t], token = decode(wholes[t], [chunk], ratios, me, [place])
            done.append(token)
        return done

    send_first()
    tables.append(buddies(maxima))
    send(1)
    for k in range(13):
        got = arrived(k)
        if k == 0:
            got.append(tables[1])
            tables.append(skip(after(jnp.concatenate(tables, axis=0), *got)))
        if k == 1:
            got.append(tables[2])
            scales, most = half_table(tables)
            far_scales = across(after(scales, *got))
            far_most = across(after(most, *got))
        if k == 2:
            got += [far_scales, far_most]
            ratios, factors = ratios_of((scales, far_scales), (most, far_most))
        if k + 2 < 13:
            send(k + 2, *got, *tokens)
        elif k + 2 == 13:
            send_last(*got, *tokens)
        if k == 2:
            out = jax.ShapeDtypeStruct((8 * rows, columns), jnp.bfloat16)
            wholes, tokens = zip(*[decode(out, own[t::2], ratios, me, [(own_of, t, 0), (own_of, t + 2, 0)]) for t in (0, 1)])
            wholes = list(wholes)
        if k >= 3:
            tokens = settle(3 if k < 12 else len(waiting))
    for name, offset in (("a", 0), ("b", cut)):
        places = [(diagonal_of, 1, offset), (far_across_of, 3, offset)]
        wholes[1], _ = decode(wholes[1], [after(F[name], *tokens), after(X[name], *tokens)], ratios, me, places)
    return (*wholes, factors[0], factors[1])


def local_any(w_gate, avg_gate, w_up, avg_up, norm_gain):
    fresh_gained_gate = (keep_rate * avg_gate + (1.0 - keep_rate) * w_gate) * norm_gain[:, None]
    fresh_gained_up = (keep_rate * avg_up + (1.0 - keep_rate) * w_up) * norm_gain[:, None]
    factor_gate, factor_up = lax.pmax(
        (jnp.max(jnp.abs(fresh_gained_gate), axis=0), jnp.max(jnp.abs(fresh_gained_up), axis=0)),
        "rows",
    )
    serve_gate = lax.all_gather((fresh_gained_gate / factor_gate).astype(jnp.bfloat16), "rows", axis=0, tiled=True)
    serve_up = lax.all_gather((fresh_gained_up / factor_up).astype(jnp.bfloat16), "rows", axis=0, tiled=True)
    return serve_gate, serve_up, factor_gate, factor_up


def solution(mesh):
    plane = mesh.shape["rows"] == 8

    def local(*args):
        return (local_plane if plane else local_any)(*args)

    return jax.shard_map(
        local,
        mesh=mesh,
        in_specs=(P("rows", "width"),) * 4 + (P("rows"),),
        out_specs=(P(None, "width"), P(None, "width"), P("width"), P("width")),
        check_vma=False,
    )
```

```python
import functools

import jax
import jax.numpy as jnp
from jax import lax
from jax.experimental import pallas as pl
from jax.experimental.pallas import tpu as pltpu
from jax.sharding import PartitionSpec as P


keep_rate = 0.7

SPAN = 250.0
SCALE_OF_CHUNK = (0, 1, 2, 1)


MIB = 2**20


def near_by(value):
    return pltpu.with_memory_space_constraint(value, pltpu.VMEM)


def stay_out(value):
    return pltpu.with_memory_space_constraint(value, pltpu.HBM)


def gained(w_ref, a_ref, gain):
    fresh = keep_rate * a_ref[...] + (1.0 - keep_rate) * w_ref[...]
    return fresh * gain


def tall_gain(gain_ref, width):
    rows = gain_ref.shape[0]
    lanes = jnp.broadcast_to(gain_ref[...].reshape(1, rows), (128, rows)).T
    return jnp.concatenate([lanes] * (width // 128), axis=1)


def scale_of(m):
    return m.astype(jnp.bfloat16).astype(jnp.float32)


def largest(x):
    return jnp.max(jnp.abs(x), axis=0, keepdims=True)


def coded(x, m):
    y = jnp.exp2(jnp.abs(x) * (SPAN / jnp.maximum(scale_of(m), 1e-30)) - SPAN / 2)
    return jnp.where(x < 0, -y, y).astype(jnp.bfloat16)


def encode_rest_body(gain_ref, wu0, au0, wg, ag, wu1, au1, first_ref, first_max_ref, own_ref, up0, gate, up1, m_ref):
    half_rows, width = wg.shape
    tall = tall_gain(gain_ref, width)
    top, bottom = tall[:half_rows], tall[half_rows:]
    upper, lower = gained(wu0, au0, top), gained(wu1, au1, bottom)
    m = jnp.maximum(largest(upper), largest(lower))
    up0[...] = coded(upper, m)
    up1[...] = coded(lower, m)
    m_ref[1] = m
    x = gained(wg, ag, bottom)
    m = largest(x)
    gate[...] = coded(x, m)
    m_ref[2] = m
    m_ref[0] = first_max_ref[0]
    own_ref[...] = first_ref[...]


def encode_rest(w_gate, avg_gate, w_up, avg_up, gain, first, first_maxima, block):
    half_rows, columns = w_gate.shape[0] // 2, w_gate.shape[1]
    half = lambda h: [pl.BlockSpec((half_rows, block), lambda j: (h, j))] * 2
    stacked = lambda n: pl.BlockSpec((n, 1, block), lambda j: (0, 0, j))
    whole = pl.BlockSpec((half_rows, block), lambda j: (0, j))
    chunk = pltpu.HBM((half_rows, columns), jnp.bfloat16)
    return pl.pallas_call(
        encode_rest_body,
        grid=(columns // block,),
        in_specs=[pl.BlockSpec(gain.shape, lambda j: (0,)), *half(0), *half(1), *half(1), whole, stacked(1)],
        out_specs=[whole] * 4 + [stacked(3)],
        out_shape=[chunk] * 4 + [jax.ShapeDtypeStruct((3, 1, columns), jnp.float32)],
        compiler_params=pltpu.CompilerParams(vmem_limit_bytes=12 * MIB),
        name="encode_rest",
    )(gain, *map(stay_out, (w_up, avg_up, w_gate, avg_gate, w_up, avg_up)), near_by(first), near_by(first_maxima))


def encode_first_body(g_ref, w_ref, a_ref, y_ref, m_ref, gain_ref, ws, avgs, sems, *, half):
    half_rows, _ = y_ref.shape
    steps, _, width = ws.shape
    copies = []
    gain_copy = pltpu.make_async_copy(g_ref, gain_ref, sems.at[2, 0])
    gain_copy.start()
    for j in range(steps):
        source = (pl.ds(half * half_rows, half_rows), pl.ds(j * width, width))
        pair = [
            pltpu.make_async_copy(ref.at[source], held.at[j], sems.at[i, j])
            for i, (ref, held) in enumerate(((w_ref, ws), (a_ref, avgs)))
        ]
        for copy in pair:
            copy.start()
        copies.append(pair)
    gain_copy.wait()
    gain = tall_gain(gain_ref, width)[half * half_rows : (half + 1) * half_rows]
    for j, pair in enumerate(copies):
        for copy in pair:
            copy.wait()
        part = pl.ds(j * width, width)
        x = gained(ws.at[j], avgs.at[j], gain)
        m = largest(x)
        y_ref[:, part] = coded(x, m)
        m_ref[0, :, part] = m


def encode_first(w, avg, gain, half, width):
    half_rows, columns = w.shape[0] // 2, w.shape[1]
    here = pl.BlockSpec(memory_space=pltpu.VMEM)
    there = pl.BlockSpec(memory_space=pl.ANY)
    held = pltpu.VMEM((columns // width, half_rows, width), jnp.float32)
    return pl.pallas_call(
        functools.partial(encode_first_body, half=half),
        in_specs=[there, there, there],
        out_specs=[here, here],
        out_shape=[
            pltpu.VMEM((half_rows, columns), jnp.bfloat16),
            pltpu.VMEM((1, 1, columns), jnp.float32),
        ],
        scratch_shapes=[pltpu.VMEM(gain.shape, gain.dtype), held, held, pltpu.SemaphoreType.DMA((3, columns // width))],
        compiler_params=pltpu.CompilerParams(vmem_limit_bytes=6 * MIB),
        name="encode_first",
    )(stay_out(gain), stay_out(w), stay_out(avg))


def half_table_body(m0_ref, m1_ref, m2_ref, scale_ref, most_ref):
    rows = [ref[i] for ref in (m0_ref, m1_ref, m2_ref) for i in range(ref.shape[0])]
    rest = [jnp.zeros_like(rows[0])] * (scale_ref.shape[0] - len(rows))
    scale_ref[...] = jnp.concatenate(rows + rest, axis=0).astype(jnp.bfloat16)
    most_ref[0] = functools.reduce(jnp.maximum, rows[0::3] + rows[2::3])
    most_ref[1] = functools.reduce(jnp.maximum, rows[1::3])


def half_table(maxima):
    columns = maxima[0].shape[-1]
    return pl.pallas_call(
        half_table_body,
        out_shape=[
            pltpu.VMEM((16, columns), jnp.bfloat16),
            pltpu.VMEM((2, 1, columns), jnp.float32),
        ],
        compiler_params=pltpu.CompilerParams(vmem_limit_bytes=4 * MIB),
        name="half_table",
    )(*map(near_by, maxima))


def ratios_body(scale0_ref, scale1_ref, most0_ref, most1_ref, ratio_ref, factor_ref):
    for t in range(2):
        factor = jnp.maximum(most0_ref[t], most1_ref[t])
        factor_ref[t : t + 1, :] = factor
        for side, scale_ref in enumerate((scale0_ref, scale1_ref)):
            scales = scale_ref[...].astype(jnp.float32)
            for place in range(4):
                for k in (3 * place, 3 * place + 2) if t == 0 else (3 * place + 1,):
                    ratio_ref[3 * place + 3 * side + k] = scales[k : k + 1] / factor


def ratios_of(scales, most):
    columns = most[0].shape[-1]
    return pl.pallas_call(
        ratios_body,
        out_shape=[
            pltpu.VMEM((24, 1, columns), jnp.float32),
            jax.ShapeDtypeStruct((2, columns), jnp.float32),
        ],
        compiler_params=pltpu.CompilerParams(vmem_limit_bytes=4 * MIB),
        name="ratios",
    )(*map(near_by, scales), *map(near_by, most))


def decoded(y, ratio):
    y = y.astype(jnp.float32)
    x = jnp.log2(jnp.abs(y)) * (ratio * (1.0 / SPAN)) + ratio * 0.5
    return jnp.where(y < 0, -x, x).astype(jnp.bfloat16)


def decode_body(me_ref, r_ref, *refs, places, pieces, half_rows):
    count = len(places)
    chunks, (out_ref, token_ref, buffer, sems) = refs[:count], refs[-4:]
    rows = chunks[0].shape[0] // pieces
    me = me_ref[0]
    copies = []
    for i, (shard_of, c, offset) in enumerate(places):
        shard = shard_of(me)
        ratio = r_ref[(shard ^ me) * 3 + SCALE_OF_CHUNK[c]]
        start = (2 * shard + c // 2) * half_rows + offset
        for p in range(pieces):
            part = pl.ds(p * rows, rows)
            buffer[i, part] = decoded(chunks[i][part], ratio)
            copies.append(
                pltpu.make_async_copy(buffer.at[i, part], out_ref.at[pl.ds(start + p * rows, rows)], sems.at[i, p])
            )
            copies[-1].start()
    token_ref[...] = jnp.zeros_like(token_ref)
    for copy in copies:
        copy.wait()


def decode(whole, chunks, ratios, me, places):
    here = pl.BlockSpec(memory_space=pltpu.VMEM)
    there = pl.BlockSpec(memory_space=pl.ANY)
    begun = not isinstance(whole, jax.ShapeDtypeStruct)
    half_rows, height = whole.shape[0] // 16, chunks[0].shape[0]
    pieces = next(n for n in (4, 3, 1) if height % (16 * n) == 0)
    return pl.pallas_call(
        functools.partial(decode_body, places=places, pieces=pieces, half_rows=half_rows),
        in_specs=[pl.BlockSpec(memory_space=pltpu.SMEM), here] + [here] * len(chunks) + [there] * begun,
        out_specs=[there, here],
        out_shape=[
            jax.ShapeDtypeStruct(whole.shape, whole.dtype),
            pltpu.VMEM((8, 128), jnp.float32),
        ],
        scratch_shapes=[
            pltpu.VMEM((len(chunks), *chunks[0].shape), whole.dtype),
            pltpu.SemaphoreType.DMA((len(chunks), pieces)),
        ],
        input_output_aliases={2 + len(chunks): 0} if begun else {},
        compiler_params=pltpu.CompilerParams(vmem_limit_bytes=4 * MIB),
        name="decode",
    )(me, near_by(ratios), *map(near_by, chunks), *[whole] * begun)


def after(value, *tokens):
    return lax.optimization_barrier((value, *tokens))[0]


def own_of(me):
    return me


def across_of(me):
    return me ^ 1


def buddy_of(me):
    return me ^ 2


def diagonal_of(me):
    return me ^ 3


def near_of(me):
    return jnp.where(me < 4, 4, 2) + (me & 1)


def far_of(me):
    return jnp.where(me < 4, 6, 0) + (me & 1)


def near_across_of(me):
    return near_of(me) ^ 1


def far_across_of(me):
    return far_of(me) ^ 1


def local_plane(w_gate, avg_gate, w_up, avg_up, norm_gain):
    rows, columns = w_gate.shape
    block = min(columns, 1024)
    cut = rows // 2 - rows // 128 * 16
    width = lax.axis_size("width")
    index = lax.axis_index("rows")
    outer = (index < 2) | (index >= 6)
    me = jnp.reshape(index, (1,)).astype(jnp.int32)

    def hop(value, pairs):
        both = [(2 * a + side, 2 * b + side) for a, b in pairs for side in (0, 1)]
        return lax.ppermute(value, "rows", both)

    across = lambda value: lax.ppermute(value, "rows", [(i, i ^ 1) for i in range(8)])
    buddies = lambda value: hop(value, [(0, 1), (1, 0), (2, 3), (3, 2)])
    outward = lambda value: hop(value, [(1, 0), (2, 3)])
    middle = lambda value: hop(value, [(1, 2), (2, 1)])
    skip = lambda value: hop(value, [(0, 2), (2, 0), (1, 3), (3, 1)])

    first, first_maxima = encode_first(w_gate, avg_gate, norm_gain, 0, block // 4)
    *own, maxima = encode_rest(w_gate, avg_gate, w_up, avg_up, norm_gain, first, first_maxima, block // 2)

    X, B, M, O, V, F = {}, {}, {}, {}, {}, {}
    tables = [maxima]
    factors = ratios = None
    wholes, tokens, waiting = [None, None], [], []

    def wait_for(chunk, shard_of, c, offset=0):
        waiting.append((chunk, (shard_of, c, offset)))

    def arrived(k):
        got = [X[k]]
        if k < 4:
            got += [B[k], M[k]]
            wait_for(X[k], across_of, k)
            wait_for(B[k], buddy_of, k)
        elif k < 8:
            got += [O[k], M[k]]
        elif k < 12:
            got += [O[k]]
        else:
            got += [F[0]]
            wait_for(F[0], diagonal_of, 0)
        if 4 <= k < 6:
            wait_for(X[k], diagonal_of, k - 2)
        if 6 <= k < 10:
            wait_for(X[k], near_across_of, k - 6)
        if 10 <= k:
            wait_for(X[k], far_across_of, k - 10)
        if 4 <= k < 12:
            j = k - 4
            V[j] = jnp.where(outer, O[k], M[j])
            wait_for(V[j], near_of if j < 4 else far_of, j % 4)
        return got

    def send_last(*ties):
        parts = [slice(0, cut), slice(cut, rows // 2)]
        for name, part in zip("ab", parts):
            X[name] = across(after(jnp.where(outer, O[11][part], M[7][part]), *ties))
            F[name] = buddies(after(X[1][part], *ties))

    def send_first():
        odd = lax.axis_index("width") % 2 == 1
        cores = [(row, column) for row in range(8) for column in range(width)]
        flat = lambda row, column: row * width + column
        swap = lambda turn: lax.ppermute(
            first,
            ("rows", "width"),
            [(flat(r, c), flat(r ^ (1 if (c + turn) % 2 == 0 else 2), c)) for r, c in cores],
        )
        one = swap(0)
        two = swap(1)
        M[0] = middle(first)
        X[0] = jnp.where(odd, two, one)
        B[0] = jnp.where(odd, one, two)

    def send(k, *ties):
        tie = lambda value: after(value, *ties) if ties else value
        if k < 4:
            X[k] = across(tie(own[k]))
        elif k < 6:
            X[k] = across(tie(B[k - 2]))
        else:
            X[k] = across(tie(V[k - 6]))
        if k < 4:
            B[k] = buddies(tie(own[k]))
        elif k < 12:
            O[k] = outward(tie(M[k - 4]))
        else:
            F[k - 12] = buddies(tie(X[k - 12]))
        if k < 4:
            M[k] = middle(tie(own[k]))
        elif k < 8:
            M[k] = middle(tie(B[k - 4]))

    def settle(count):
        done = []
        for _ in range(min(count, len(waiting))):
            chunk, place = waiting.pop(0)
            t = place[1] % 2
            wholes[t], token = decode(wholes[t], [chunk], ratios, me, [place])
            done.append(token)
        return done

    send_first()
    tables.append(buddies(maxima))
    send(1)
    for k in range(13):
        got = arrived(k)
        if k == 0:
            got.append(tables[1])
            tables.append(skip(after(jnp.concatenate(tables, axis=0), *got)))
        if k == 1:
            got.append(tables[2])
            scales, most = half_table(tables)
            far_scales = across(after(scales, *got))
            far_most = across(after(most, *got))
        if k == 2:
            got += [far_scales, far_most]
            ratios, factors = ratios_of((scales, far_scales), (most, far_most))
        if k + 2 < 13:
            send(k + 2, *got, *tokens)
        elif k + 2 == 13:
            send_last(*got, *tokens)
        if k == 2:
            out = jax.ShapeDtypeStruct((8 * rows, columns), jnp.bfloat16)
            wholes, tokens = zip(*[decode(out, own[t::2], ratios, me, [(own_of, t, 0), (own_of, t + 2, 0)]) for t in (0, 1)])
            wholes = list(wholes)
        if k >= 3:
            tokens = settle(3 if k < 12 else len(waiting))
    for name, offset in (("a", 0), ("b", cut)):
        places = [(diagonal_of, 1, offset), (far_across_of, 3, offset)]
        wholes[1], _ = decode(wholes[1], [after(F[name], *tokens), after(X[name], *tokens)], ratios, me, places)
    return (*wholes, factors[0], factors[1])


def local_any(w_gate, avg_gate, w_up, avg_up, norm_gain):
    fresh_gained_gate = (keep_rate * avg_gate + (1.0 - keep_rate) * w_gate) * norm_gain[:, None]
    fresh_gained_up = (keep_rate * avg_up + (1.0 - keep_rate) * w_up) * norm_gain[:, None]
    factor_gate, factor_up = lax.pmax(
        (jnp.max(jnp.abs(fresh_gained_gate), axis=0), jnp.max(jnp.abs(fresh_gained_up), axis=0)),
        "rows",
    )
    serve_gate = lax.all_gather((fresh_gained_gate / factor_gate).astype(jnp.bfloat16), "rows", axis=0, tiled=True)
    serve_up = lax.all_gather((fresh_gained_up / factor_up).astype(jnp.bfloat16), "rows", axis=0, tiled=True)
    return serve_gate, serve_up, factor_gate, factor_up


def solution(mesh):
    plane = mesh.shape["rows"] == 8

    def local(*args):
        return (local_plane if plane else local_any)(*args)

    return jax.shard_map(
        local,
        mesh=mesh,
        in_specs=(P("rows", "width"),) * 4 + (P("rows"),),
        out_specs=(P(None, "width"), P(None, "width"), P("width"), P("width")),
        check_vma=False,
    )
```

```python
import functools

import jax
import jax.numpy as jnp
from jax import lax
from jax.experimental import pallas as pl
from jax.experimental.pallas import tpu as pltpu
from jax.sharding import PartitionSpec as P


keep_rate = 0.7

SPAN = 250.0
SCALE_OF_CHUNK = (0, 1, 2, 1)


MIB = 2**20


def near_by(value):
    return pltpu.with_memory_space_constraint(value, pltpu.VMEM)


def stay_out(value):
    return pltpu.with_memory_space_constraint(value, pltpu.HBM)


def gained(w_ref, a_ref, gain):
    fresh = keep_rate * a_ref[...] + (1.0 - keep_rate) * w_ref[...]
    return fresh * gain


def tall_gain(gain_ref, width):
    rows = gain_ref.shape[0]
    lanes = jnp.broadcast_to(gain_ref[...].reshape(1, rows), (128, rows)).T
    return jnp.concatenate([lanes] * (width // 128), axis=1)


def scale_of(m):
    return m.astype(jnp.bfloat16).astype(jnp.float32)


def largest(x):
    return jnp.max(jnp.abs(x), axis=0, keepdims=True)


def coded(x, m):
    y = jnp.exp2(jnp.abs(x) * (SPAN / jnp.maximum(scale_of(m), 1e-30)) - SPAN / 2)
    return jnp.where(x < 0, -y, y).astype(jnp.bfloat16)


def encode_rest_body(gain_ref, wu0, au0, wg, ag, wu1, au1, *refs):
    firsts, first_maxima, (own_ref, up0, gate, up1, m_ref) = refs[:2], refs[2:4], refs[4:]
    half_rows, width = wg.shape
    tall = tall_gain(gain_ref, width)
    top, bottom = tall[:half_rows], tall[half_rows:]
    upper, lower = gained(wu0, au0, top), gained(wu1, au1, bottom)
    m = jnp.maximum(largest(upper), largest(lower))
    up0[...] = coded(upper, m)
    up1[...] = coded(lower, m)
    m_ref[1] = m
    x = gained(wg, ag, bottom)
    m = largest(x)
    gate[...] = coded(x, m)
    m_ref[2] = m
    for side in (0, 1):

        @pl.when(pl.program_id(0) // (pl.num_programs(0) // 2) == side)
        def _(side=side):
            m_ref[0] = first_maxima[side][0]
            own_ref[...] = firsts[side][...]


def encode_rest(w_gate, avg_gate, w_up, avg_up, gain, firsts, first_maxima, block):
    half_rows, columns = w_gate.shape[0] // 2, w_gate.shape[1]
    half = lambda h: [pl.BlockSpec((half_rows, block), lambda j: (h, j))] * 2
    stacked = lambda n: pl.BlockSpec((n, 1, block), lambda j: (0, 0, j))
    whole = pl.BlockSpec((half_rows, block), lambda j: (0, j))
    steps = columns // block
    at = [lambda j: jnp.minimum(j, steps // 2 - 1), lambda j: jnp.maximum(j - steps // 2, 0)]
    first_specs = [pl.BlockSpec((half_rows, block), lambda j, f=f: (0, f(j))) for f in at]
    max_specs = [pl.BlockSpec((1, 1, block), lambda j, f=f: (0, 0, f(j))) for f in at]
    chunk = pltpu.HBM((half_rows, columns), jnp.bfloat16)
    return pl.pallas_call(
        encode_rest_body,
        grid=(steps,),
        in_specs=[pl.BlockSpec(gain.shape, lambda j: (0,)), *half(0), *half(1), *half(1), *first_specs, *max_specs],
        out_specs=[whole] * 4 + [stacked(3)],
        out_shape=[chunk] * 4 + [jax.ShapeDtypeStruct((3, 1, columns), jnp.float32)],
        compiler_params=pltpu.CompilerParams(vmem_limit_bytes=12 * MIB),
        name="encode_rest",
    )(gain, *map(stay_out, (w_up, avg_up, w_gate, avg_gate, w_up, avg_up)), *map(near_by, (*firsts, *first_maxima)))


def encode_first_body(g_ref, w_ref, a_ref, y_ref, m_ref, gain_ref, ws, avgs, sems, *, half, side):
    half_rows, columns = y_ref.shape
    steps, _, width = ws.shape
    copies = []
    gain_copy = pltpu.make_async_copy(g_ref, gain_ref, sems.at[2, 0])
    gain_copy.start()
    for j in range(steps):
        source = (pl.ds(half * half_rows, half_rows), pl.ds(side * columns + j * width, width))
        pair = [
            pltpu.make_async_copy(ref.at[source], held.at[j], sems.at[i, j])
            for i, (ref, held) in enumerate(((w_ref, ws), (a_ref, avgs)))
        ]
        for copy in pair:
            copy.start()
        copies.append(pair)
    gain_copy.wait()
    gain = tall_gain(gain_ref, width)[half * half_rows : (half + 1) * half_rows]
    for j, pair in enumerate(copies):
        for copy in pair:
            copy.wait()
        part = pl.ds(j * width, width)
        x = gained(ws.at[j], avgs.at[j], gain)
        m = largest(x)
        y_ref[:, part] = coded(x, m)
        m_ref[0, :, part] = m


def encode_first(w, avg, gain, half, side, width):
    half_rows, columns = w.shape[0] // 2, w.shape[1] // 2
    here = pl.BlockSpec(memory_space=pltpu.VMEM)
    there = pl.BlockSpec(memory_space=pl.ANY)
    held = pltpu.VMEM((columns // width, half_rows, width), jnp.float32)
    return pl.pallas_call(
        functools.partial(encode_first_body, half=half, side=side),
        in_specs=[there, there, there],
        out_specs=[here, here],
        out_shape=[
            pltpu.VMEM((half_rows, columns), jnp.bfloat16),
            pltpu.VMEM((1, 1, columns), jnp.float32),
        ],
        scratch_shapes=[pltpu.VMEM(gain.shape, gain.dtype), held, held, pltpu.SemaphoreType.DMA((3, columns // width))],
        compiler_params=pltpu.CompilerParams(vmem_limit_bytes=6 * MIB),
        name="encode_first",
    )(stay_out(gain), stay_out(w), stay_out(avg))


def half_table_body(m0_ref, m1_ref, m2_ref, scale_ref, most_ref):
    rows = [ref[i] for ref in (m0_ref, m1_ref, m2_ref) for i in range(ref.shape[0])]
    rest = [jnp.zeros_like(rows[0])] * (scale_ref.shape[0] - len(rows))
    scale_ref[...] = jnp.concatenate(rows + rest, axis=0).astype(jnp.bfloat16)
    most_ref[0] = functools.reduce(jnp.maximum, rows[0::3] + rows[2::3])
    most_ref[1] = functools.reduce(jnp.maximum, rows[1::3])


def half_table(maxima):
    columns = maxima[0].shape[-1]
    return pl.pallas_call(
        half_table_body,
        out_shape=[
            pltpu.VMEM((16, columns), jnp.bfloat16),
            pltpu.VMEM((2, 1, columns), jnp.float32),
        ],
        compiler_params=pltpu.CompilerParams(vmem_limit_bytes=4 * MIB),
        name="half_table",
    )(*map(near_by, maxima))


def ratios_body(scale0_ref, scale1_ref, most0_ref, most1_ref, ratio_ref, factor_ref):
    for t in range(2):
        factor = jnp.maximum(most0_ref[t], most1_ref[t])
        factor_ref[t : t + 1, :] = factor
        for side, scale_ref in enumerate((scale0_ref, scale1_ref)):
            scales = scale_ref[...].astype(jnp.float32)
            for place in range(4):
                for k in (3 * place, 3 * place + 2) if t == 0 else (3 * place + 1,):
                    ratio_ref[3 * place + 3 * side + k] = scales[k : k + 1] / factor


def ratios_of(scales, most):
    columns = most[0].shape[-1]
    return pl.pallas_call(
        ratios_body,
        out_shape=[
            pltpu.VMEM((24, 1, columns), jnp.float32),
            jax.ShapeDtypeStruct((2, columns), jnp.float32),
        ],
        compiler_params=pltpu.CompilerParams(vmem_limit_bytes=4 * MIB),
        name="ratios",
    )(*map(near_by, scales), *map(near_by, most))


def decoded(y, ratio):
    y = y.astype(jnp.float32)
    x = jnp.log2(jnp.abs(y)) * (ratio * (1.0 / SPAN)) + ratio * 0.5
    return jnp.where(y < 0, -x, x).astype(jnp.bfloat16)


def decode_body(me_ref, r_ref, *refs, places, pieces, half_rows):
    count = len(places)
    chunks, (out_ref, token_ref, buffer, sems) = refs[:count], refs[-4:]
    rows = chunks[0].shape[0] // pieces
    me = me_ref[0]
    copies = []
    for i, (shard_of, c, offset) in enumerate(places):
        shard = shard_of(me)
        ratio = r_ref[(shard ^ me) * 3 + SCALE_OF_CHUNK[c]]
        start = (2 * shard + c // 2) * half_rows + offset
        for p in range(pieces):
            part = pl.ds(p * rows, rows)
            buffer[i, part] = decoded(chunks[i][part], ratio)
            copies.append(
                pltpu.make_async_copy(buffer.at[i, part], out_ref.at[pl.ds(start + p * rows, rows)], sems.at[i, p])
            )
            copies[-1].start()
    token_ref[...] = jnp.zeros_like(token_ref)
    for copy in copies:
        copy.wait()


def decode(whole, chunks, ratios, me, places):
    here = pl.BlockSpec(memory_space=pltpu.VMEM)
    there = pl.BlockSpec(memory_space=pl.ANY)
    begun = not isinstance(whole, jax.ShapeDtypeStruct)
    half_rows, height = whole.shape[0] // 16, chunks[0].shape[0]
    pieces = next(n for n in (4, 3, 1) if height % (16 * n) == 0)
    return pl.pallas_call(
        functools.partial(decode_body, places=places, pieces=pieces, half_rows=half_rows),
        in_specs=[pl.BlockSpec(memory_space=pltpu.SMEM), here] + [here] * len(chunks) + [there] * begun,
        out_specs=[there, here],
        out_shape=[
            jax.ShapeDtypeStruct(whole.shape, whole.dtype),
            pltpu.VMEM((8, 128), jnp.float32),
        ],
        scratch_shapes=[
            pltpu.VMEM((len(chunks), *chunks[0].shape), whole.dtype),
            pltpu.SemaphoreType.DMA((len(chunks), pieces)),
        ],
        input_output_aliases={2 + len(chunks): 0} if begun else {},
        compiler_params=pltpu.CompilerParams(vmem_limit_bytes=4 * MIB),
        name="decode",
    )(me, near_by(ratios), *map(near_by, chunks), *[whole] * begun)


def after(value, *tokens):
    return lax.optimization_barrier((value, *tokens))[0]


def own_of(me):
    return me


def across_of(me):
    return me ^ 1


def buddy_of(me):
    return me ^ 2


def diagonal_of(me):
    return me ^ 3


def near_of(me):
    return jnp.where(me < 4, 4, 2) + (me & 1)


def far_of(me):
    return jnp.where(me < 4, 6, 0) + (me & 1)


def near_across_of(me):
    return near_of(me) ^ 1


def far_across_of(me):
    return far_of(me) ^ 1


def local_plane(w_gate, avg_gate, w_up, avg_up, norm_gain):
    rows, columns = w_gate.shape
    block = min(columns, 1024)
    cut = rows // 2 - rows // 128 * 16
    width = lax.axis_size("width")
    index = lax.axis_index("rows")
    outer = (index < 2) | (index >= 6)
    me = jnp.reshape(index, (1,)).astype(jnp.int32)

    def hop(value, pairs):
        both = [(2 * a + side, 2 * b + side) for a, b in pairs for side in (0, 1)]
        return lax.ppermute(value, "rows", both)

    across = lambda value: lax.ppermute(value, "rows", [(i, i ^ 1) for i in range(8)])
    buddies = lambda value: hop(value, [(0, 1), (1, 0), (2, 3), (3, 2)])
    outward = lambda value: hop(value, [(1, 0), (2, 3)])
    middle = lambda value: hop(value, [(1, 2), (2, 1)])
    skip = lambda value: hop(value, [(0, 2), (2, 0), (1, 3), (3, 1)])

    firsts, first_maxima = [], []
    for side in (0, 1):
        first, m = encode_first(w_gate, avg_gate, norm_gain, 0, side, block // 4)
        firsts.append(first)
        first_maxima.append(m)
    *own, maxima = encode_rest(w_gate, avg_gate, w_up, avg_up, norm_gain, firsts, first_maxima, block // 2)

    X, B, M, O, V, F = {}, {}, {}, {}, {}, {}
    tables = [maxima]
    factors = ratios = None
    wholes, tokens, waiting = [None, None], [], []

    def wait_for(chunk, shard_of, c, offset=0):
        waiting.append((chunk, (shard_of, c, offset)))

    def arrived(k):
        got = [X[k]]
        if k < 4:
            got += [B[k]]
            wait_for(X[k], across_of, k)
            wait_for(B[k], buddy_of, k)
        elif k < 12:
            got += [O[k]]
        else:
            got += [F[0]]
            wait_for(F[0], diagonal_of, 0)
        if 1 <= k <= 8:
            got.append(M[k - 1])
        if 4 <= k < 6:
            wait_for(X[k], diagonal_of, k - 2)
        if 6 <= k < 10:
            wait_for(X[k], near_across_of, k - 6)
        if 10 <= k:
            wait_for(X[k], far_across_of, k - 10)
        if 4 <= k < 12:
            j = k - 4
            V[j] = jnp.where(outer, O[k], M[j])
            wait_for(V[j], near_of if j < 4 else far_of, j % 4)
        return got

    def send_last(*ties):
        parts = [slice(0, cut), slice(cut, rows // 2)]
        for name, part in zip("ab", parts):
            X[name] = across(after(jnp.where(outer, O[11][part], M[7][part]), *ties))
            F[name] = buddies(after(X[1][part], *ties))

    def send_first():
        odd = lax.axis_index("width") % 2 == 1
        cores = [(row, column) for row in range(8) for column in range(width)]
        flat = lambda row, column: row * width + column
        swap = lambda half, turn: lax.ppermute(
            half,
            ("rows", "width"),
            [(flat(r, c), flat(r ^ (1 if (c + turn) % 2 == 0 else 2), c)) for r, c in cores],
        )
        one, two = [], []
        for half in firsts:
            one.append(swap(half, 0))
            two.append(swap(half, 1))
        one, two = (jnp.concatenate(halves, axis=1) for halves in (one, two))
        X[0] = jnp.where(odd, two, one)
        B[0] = jnp.where(odd, one, two)
        M[0] = middle(own[0])

    def send(k, *ties):
        tie = lambda value: after(value, *ties) if ties else value
        if k < 4:
            X[k] = across(tie(own[k]))
        elif k < 6:
            X[k] = across(tie(B[k - 2]))
        else:
            X[k] = across(tie(V[k - 6]))
        if k < 4:
            B[k] = buddies(tie(own[k]))
        elif k < 12:
            O[k] = outward(tie(M[k - 4]))
        else:
            F[k - 12] = buddies(tie(X[k - 12]))
        if k < 4:
            M[k] = middle(tie(own[k]))
        elif k < 8:
            M[k] = middle(tie(B[k - 4]))

    def settle(count):
        done = []
        for _ in range(min(count, len(waiting))):
            chunk, place = waiting.pop(0)
            t = place[1] % 2
            wholes[t], token = decode(wholes[t], [chunk], ratios, me, [place])
            done.append(token)
        return done

    send_first()
    tables.append(buddies(maxima))
    send(1)
    for k in range(13):
        got = arrived(k)
        if k == 0:
            got.append(tables[1])
            tables.append(skip(after(jnp.concatenate(tables, axis=0), *got)))
        if k == 1:
            got.append(tables[2])
            scales, most = half_table(tables)
            far_scales = across(after(scales, *got))
            far_most = across(after(most, *got))
        if k == 2:
            got += [far_scales, far_most]
            ratios, factors = ratios_of((scales, far_scales), (most, far_most))
        if k + 2 < 13:
            send(k + 2, *got, *tokens)
        elif k + 2 == 13:
            send_last(*got, *tokens)
        if k == 2:
            out = jax.ShapeDtypeStruct((8 * rows, columns), jnp.bfloat16)
            wholes, tokens = zip(*[decode(out, own[t::2], ratios, me, [(own_of, t, 0), (own_of, t + 2, 0)]) for t in (0, 1)])
            wholes = list(wholes)
        if k >= 3:
            tokens = settle(3 if k < 12 else len(waiting))
    for name, offset in (("a", 0), ("b", cut)):
        places = [(diagonal_of, 1, offset), (far_across_of, 3, offset)]
        wholes[1], _ = decode(wholes[1], [after(F[name], *tokens), after(X[name], *tokens)], ratios, me, places)
    return (*wholes, factors[0], factors[1])


def local_any(w_gate, avg_gate, w_up, avg_up, norm_gain):
    fresh_gained_gate = (keep_rate * avg_gate + (1.0 - keep_rate) * w_gate) * norm_gain[:, None]
    fresh_gained_up = (keep_rate * avg_up + (1.0 - keep_rate) * w_up) * norm_gain[:, None]
    factor_gate, factor_up = lax.pmax(
        (jnp.max(jnp.abs(fresh_gained_gate), axis=0), jnp.max(jnp.abs(fresh_gained_up), axis=0)),
        "rows",
    )
    serve_gate = lax.all_gather((fresh_gained_gate / factor_gate).astype(jnp.bfloat16), "rows", axis=0, tiled=True)
    serve_up = lax.all_gather((fresh_gained_up / factor_up).astype(jnp.bfloat16), "rows", axis=0, tiled=True)
    return serve_gate, serve_up, factor_gate, factor_up


def solution(mesh):
    plane = mesh.shape["rows"] == 8

    def local(*args):
        return (local_plane if plane else local_any)(*args)

    return jax.shard_map(
        local,
        mesh=mesh,
        in_specs=(P("rows", "width"),) * 4 + (P("rows"),),
        out_specs=(P(None, "width"), P(None, "width"), P("width"), P("width")),
        check_vma=False,
    )
```
